128 devices in a mesh: edp: 2 (over z_lo), ep: 64 (over z_hi, x, y, core).
Axes of the slice: x: 4, y: 4, z: 4 (z_hi: 2, z_lo: 2; z = z_hi * 2 + z_lo), core: 2. Of those that a mesh axis runs over, the one named last changes fastest.
Arguments:
- tokens: bfloat16 [16384, 3584], P(('edp', 'ep')), may hold values from -6 to 6
- node_ids: int32 [16384, 4], P(('edp', 'ep')), may hold values from 0 to 7, as said below
- local_ids: int32 [16384, 8], P(('edp', 'ep')), may hold values from 0 to 15, as said below
- affinity: float32 [16384, 8], P(('edp', 'ep')), may hold values from 0.2 to 1
- w_gate: bfloat16 [128, 3584, 1024], P(('edp', 'ep')), may hold values from -0.09375 to 0.09375
- w_up: bfloat16 [128, 3584, 1024], P(('edp', 'ep')), may hold values from -0.09375 to 0.09375
- w_down: bfloat16 [128, 1024, 3584], P(('edp', 'ep')), may hold values from -0.1875 to 0.1875
- grad_parts: float32 [128, 3584, 128], P(('edp', 'ep')), may hold values from -2.5 to 2.5
Outputs:
- mixed: bfloat16 [16384, 3584], P(('edp', 'ep'))
- router_grad: float32 [3584, 128], P(('edp', 'ep'))
The draws below stay inside these ranges and needn't reach their ends.
Inputs may be any that keep to these rules, and one draw needn't show every extreme that they name: `node_ids`: A token's 4 nodes are distinct and increasing. `local_ids`: columns 2 j and 2 j + 1 name the two experts 2 m and 2 m + 1 of one pair m of node node_ids[t, j], in either order. From the 128 tokens of one device each expert receives at most 10 routes; inside a node the loads from one device differ by at most one.
All inputs are finite; a program needn't handle non-finite values.
Results may differ from the reference program's by a relative error of at most 0.0057.
Values may be sent and summed in bfloat16 or wider, within the bound.
A program may use at most 192 MiB of HBM per device.

```python
import math
import jax
import jax.numpy as jnp
from jax import lax

D = 3584
H = 1024
TOK_DEV = 128
TOP = 8
NODE_PICK = 4
GROUPS = 8
EXPERTS = 128
CAP = 10
TOKENS = 16384
N_EDP = 2
N_EP = 64


def routing_plan(key):
    base_key = jax.random.fold_in(key, 7)
    per_node = EXPERTS // GROUPS
    pair_count = per_node // 2
    pairing = jax.random.permutation(jax.random.fold_in(base_key, 1), GROUPS).astype(jnp.int32)

    def block_plan(block):
        block_key = jax.random.fold_in(base_key, block + 100)
        shifts = jax.random.randint(jax.random.fold_in(block_key, 1), (GROUPS // 2,), 0, TOK_DEV // 8 + 1).astype(jnp.int32)
        shifts = shifts.at[0].set(TOK_DEV // 8)
        counts = jnp.zeros((GROUPS,), jnp.int32)
        counts = counts.at[pairing[0::2]].set(TOK_DEV // 2 + shifts)
        counts = counts.at[pairing[1::2]].set(TOK_DEV // 2 - shifts)
        node_major = jnp.repeat(jnp.arange(GROUPS, dtype=jnp.int32), counts, total_repeat_length=NODE_PICK * TOK_DEV)
        chosen = node_major.reshape(NODE_PICK, TOK_DEV).T
        shuffle = jax.random.permutation(jax.random.fold_in(block_key, 2), TOK_DEV)
        chosen = chosen[shuffle]
        onehot = jnp.sum((chosen[:, :, None] == jnp.arange(GROUPS, dtype=jnp.int32)[None, None, :]).astype(jnp.int32), axis=1)
        earlier = jnp.cumsum(onehot, axis=0) - onehot
        ranks = jnp.take_along_axis(earlier, chosen, axis=1)
        offsets = jax.random.randint(jax.random.fold_in(block_key, 3), (GROUPS,), 0, pair_count).astype(jnp.int32)
        pair_index = (ranks + offsets[chosen]) % pair_count
        flips = jax.random.randint(jax.random.fold_in(block_key, 4), (TOK_DEV, NODE_PICK), 0, 2).astype(jnp.int32)
        first = 2 * pair_index + flips
        second = 2 * pair_index + 1 - flips
        local = jnp.stack([first, second], axis=2).reshape(TOK_DEV, TOP)
        return (chosen, local)
    nodes, locals_all = jax.vmap(block_plan)(jnp.arange(EXPERTS, dtype=jnp.int32))
    return (nodes.reshape(-1, NODE_PICK).astype(jnp.int32), locals_all.reshape(-1, TOP).astype(jnp.int32))


def draw_node_ids(key, part):
    return routing_plan(key)[0]


def draw_local_ids(key, part):
    return routing_plan(key)[1]


def with_spikes(entries, rng, source, target, blocks, factor):
    def block_of(position):
        return (jnp.arange(entries.shape[position]) // (entries.shape[position] // blocks)).reshape((-1,) + (1,) * (entries.ndim - 1 - position))

    near = jax.random.permutation(rng, blocks)[block_of(target)]
    far = (block_of(target) + blocks // 2) % blocks
    return jnp.where((block_of(source) == near) | (block_of(source) == far), factor * entries, entries)


def level_of(stream_key, dims, split, least, high):
    factor_of, own = 1.0, jax.random.fold_in(stream_key, 6)
    for axis_at, shards_of in split:
        steps = jnp.exp(jax.random.uniform(jax.random.fold_in(own, axis_at), (shards_of,), jnp.float32, least / len(split), high / len(split)))
        factor_of = factor_of * jnp.repeat(steps, dims[axis_at] // shards_of).reshape([-1 if axis == axis_at else 1 for axis in range(len(dims))])
    return factor_of


def bell_draw(stream_key, shape, spread, most, split=(), held_as=jnp.bfloat16):
    level = level_of(stream_key, shape, split, -0.22, 0.18) if split else 1.0
    values = jax.random.normal(stream_key, shape, jnp.float32) * spread * level
    return jnp.minimum(jnp.maximum(values, -most), most).astype(held_as)


def bell_draw_with(stream_key, dims, scale, limit, shards, heavy, kind=jnp.bfloat16):
    entries = scale * jax.random.normal(stream_key, dims, jnp.float32)
    if shards:
        entries = entries * level_of(stream_key, dims, shards, -0.22, 0.18)
    return jnp.clip(with_spikes(entries, jax.random.fold_in(stream_key, 3), *heavy), -limit, limit).astype(kind)


def setup_inputs(seed: int = 0) -> dict:
    keys = jax.random.split(jax.random.key(seed), 9)
    tokens = bell_draw(keys[0], (TOKENS, D), 1.0, 6.0, ((0, 128),))
    node_ids = draw_node_ids(jax.random.fold_in(keys[8], 71), 0)
    local_ids = draw_local_ids(jax.random.fold_in(keys[8], 71), 0)
    affinity = jnp.clip(jnp.exp(math.log(1.0) - 1.609438 * jax.random.uniform(keys[3], (TOKENS, TOP), jnp.float32) ** level_of(keys[3], (TOKENS, TOP), ((0, 128),), -0.2, 0.2)), 0.2, 1.0)
    w_gate = bell_draw(keys[4], (EXPERTS, D, H), D ** -0.5, 0.09375, ((0, 128),))
    w_up = bell_draw(keys[5], (EXPERTS, D, H), D ** -0.5, 0.09375, ((0, 128),))
    w_down = bell_draw(keys[6], (EXPERTS, H, D), H ** -0.5, 0.1875, ((0, 128),))
    grad_parts = bell_draw_with(keys[7], (N_EDP * N_EP, D, EXPERTS), 0.1, 2.5, ((0, 128),), (0, 1, 128, 5.5), jnp.float32)
    return {"tokens": tokens, "node_ids": node_ids, "local_ids": local_ids, "affinity": affinity, "w_gate": w_gate, "w_up": w_up, "w_down": w_down, "grad_parts": grad_parts}


def reference(tokens, node_ids, local_ids, affinity, w_gate, w_up, w_down, grad_parts):
    per_node = EXPERTS // GROUPS
    expert = (jnp.repeat(node_ids, 2, axis=1) * per_node + local_ids).astype(jnp.int32)
    weight = 2.5 * affinity / jnp.sum(affinity, axis=1, keepdims=True)
    flat_expert = expert.reshape(-1)
    route_order = jnp.argsort(flat_expert, stable=True).astype(jnp.int32)
    counts = jnp.bincount(flat_expert, length=EXPERTS).astype(jnp.int32)
    starts = (jnp.cumsum(counts) - counts).astype(jnp.int32)
    rows_most = CAP * N_EDP * N_EP
    padded_order = jnp.concatenate([route_order, jnp.zeros((rows_most,), jnp.int32)])
    flat_weight = weight.reshape(-1)

    def per_expert(accum, inputs):
        gate_w, up_w, down_w, start, count = inputs
        row_index = lax.dynamic_slice(padded_order, (start.astype(jnp.int32),), (rows_most,))
        is_valid = jnp.arange(rows_most, dtype=jnp.int32) < count
        token_index = row_index // TOP
        row_block = tokens[token_index]
        gate_act = jnp.dot(row_block, gate_w, preferred_element_type=jnp.float32)
        up_act = jnp.dot(row_block, up_w, preferred_element_type=jnp.float32)
        hidden = (jax.nn.silu(gate_act) * up_act).astype(jnp.bfloat16)
        result = jnp.dot(hidden, down_w, preferred_element_type=jnp.float32).astype(jnp.bfloat16)
        scaled = jnp.where(is_valid, flat_weight[row_index], jnp.zeros((), jnp.float32))
        accum = accum.at[token_index].add(scaled[:, None] * result.astype(jnp.float32))
        return accum, None

    start_sum = jnp.zeros(tokens.shape, jnp.float32)
    mixed_sum, _ = lax.scan(per_expert, start_sum, (w_gate, w_up, w_down, starts, counts))
    router_grad = jnp.sum(grad_parts, axis=0)
    return mixed_sum.astype(jnp.bfloat16), router_grad
```

```python
import functools

import jax
import jax.numpy as jnp
from jax import lax
from jax.experimental import pallas as pl
from jax.experimental.pallas import tpu as pltpu
from jax.sharding import PartitionSpec as P

MESH = pl.DeviceIdType.MESH
CHUNKS = 2
CHIPS = 64
PER = CHIPS // CHUNKS
CAP = 10
EXT = 128
TILE = 256
BF16 = jnp.bfloat16
F32 = jnp.float32


def place():
    edp = lax.axis_index("edp")
    ep = lax.axis_index("ep")
    return (ep // 8) % 4, (ep // 2) % 4, (ep // 32) * 2 + edp, ep % 2


def device(x, y, z, core):
    x, y, z = x % 4, y % 4, z % 4
    return {"edp": z % 2, "ep": (z // 2) * 32 + x * 8 + y * 2 + core}


def offset_of(chunk, q):
    many = 4 // CHUNKS
    dx, dy = q // (4 * many), (q // many) % 4
    dz = (q % many) * CHUNKS + (chunk + 8 - dx - dy) % CHUNKS
    return dx, dy, dz


def prep_body(pos, nodes, locals_, aff, tokens, send, hot, rows, sems):
    x, y, z = pos[0], pos[1], pos[2]
    count = tokens.shape[0]
    width = tokens.shape[1]
    slots = CHIPS * CAP
    affinity = aff[...]
    weight = 2.5 * affinity / jnp.sum(affinity, axis=1, keepdims=True)
    node, local = nodes[...], locals_[...]
    lane = lax.broadcasted_iota(jnp.int32, (count, 128), 1)
    many = 4 // CHUNKS
    offsets = []
    hit = jnp.zeros((count, 128), F32)
    for j in range(4):
        pair = node[:, j : j + 1] * 8 + (local[:, 2 * j : 2 * j + 1] >> 1)
        pz = ((pair >> 4) & 1) * 2 + (pair >> 5)
        dx = (((pair >> 2) & 3) - x + 4) & 3
        dy = ((pair & 3) - y + 4) & 3
        dz = (pz - z + 4) & 3
        chunk = (dx + dy + dz) & (CHUNKS - 1)
        off = chunk * PER + (dx * 4 + dy) * many + (dz // CHUNKS)
        offsets.append(off)
        hit = hit + (lane == off).astype(F32)
    row = lax.broadcasted_iota(jnp.int32, (count, count), 0)
    col = lax.broadcasted_iota(jnp.int32, (count, count), 1)
    earlier = (col < row).astype(F32).astype(BF16)
    before = jnp.dot(earlier, hit.astype(BF16), preferred_element_type=F32)
    slot_id = lax.broadcasted_iota(jnp.int32, (count, slots), 1)
    total = jnp.zeros((count, slots), F32)
    ext = jnp.zeros((slots, EXT), F32)
    dims = (((0,), (0,)), ((), ()))
    for j in range(4):
        rank = jnp.sum(jnp.where(lane == offsets[j], before, 0.0), axis=1, keepdims=True)
        slot = offsets[j] * CAP + rank.astype(jnp.int32)
        mine = (slot_id == slot).astype(F32)
        total = total + mine
        lead_even = (local[:, 2 * j : 2 * j + 1] & 1) == 0
        first, second = weight[:, 2 * j : 2 * j + 1], weight[:, 2 * j + 1 : 2 * j + 2]
        pieces = jnp.zeros((count, EXT), F32)
        for k, value in enumerate(
            (jnp.where(lead_even, first, second), jnp.where(lead_even, second, first))
        ):
            for part in range(3):
                piece = value.astype(BF16).astype(F32)
                pieces = jnp.where(lane == 3 * k + part, piece, pieces)
                value = value - piece
        ext = ext + lax.dot_general(
            mine.astype(BF16), pieces.astype(BF16), dims, preferred_element_type=F32
        )
    one_hot = total.astype(BF16)
    hot[...] = one_hot
    rows[:, width:] = ext.astype(BF16)
    part = width // 4
    for k in range(4):
        rows[:, k * part : (k + 1) * part] = lax.dot_general(
            one_hot, tokens[:, k * part : (k + 1) * part], dims, preferred_element_type=F32
        ).astype(BF16)
    copy = pltpu.make_async_copy(rows, send.reshape(slots, width + EXT), sems)
    copy.start()
    copy.wait()


def moe_body(
    send, w_gate, w_up, w_down, land, pair_out, back,
    gate_v, up_v, down_v, xs, hidden, theirs, mine, other, summed,
    w_sems, disp_send, disp_recv, local_sems, fwd_send, fwd_recv, x_sems,
    out_send, out_recv, p_sems, back_send, back_recv,
):
    x, y, z, core = place()
    width = w_gate.shape[1]
    half = PER * CAP
    partner = {"edp": lax.axis_index("edp"), "ep": lax.axis_index("ep") + 1 - 2 * core}

    loads = [
        pltpu.make_async_copy(w_gate.at[0], gate_v, w_sems.at[0]),
        pltpu.make_async_copy(w_up.at[0], up_v, w_sems.at[1]),
        pltpu.make_async_copy(w_down.at[0], down_v, w_sems.at[2]),
    ]
    for load in loads:
        load.start()

    barrier = pltpu.get_barrier_semaphore()

    def greet(n, carry):
        pl.semaphore_signal(
            barrier, 1, device_id=device(x + n // 16, y + n // 4, z + n, core), device_id_type=MESH
        )
        return carry

    lax.fori_loop(1, CHIPS, greet, 0)
    pl.semaphore_signal(barrier, 1, device_id=partner, device_id_type=MESH)
    pl.semaphore_wait(barrier, CHIPS)

    own = pltpu.make_async_copy(send.at[0, 0], land.at[0, 0], local_sems.at[0])
    own.start()

    def dispatch(chunk, first):
        def step(q, carry):
            dx, dy, dz = offset_of(chunk, q)
            pltpu.make_async_remote_copy(
                send.at[chunk, q], land.at[chunk, q], disp_send.at[chunk], disp_recv.at[chunk],
                device_id=device(x + dx, y + dy, z + dz, core), device_id_type=MESH,
            ).start()
            return carry

        lax.fori_loop(first, PER, step, 0)

    for chunk in range(CHUNKS):
        dispatch(chunk, 1 if chunk == 0 else 0)

    def many(ref, sem):
        return pltpu.make_async_copy(ref, ref, sem)

    forwards, swaps = [], []
    for chunk in range(CHUNKS):
        first = 1 if chunk == 0 else 0
        if chunk == 0:
            own.wait()
        got = land.at[chunk, pl.ds(first, PER - first)]
        many(got, disp_recv.at[chunk]).wait()
        rows_in = land.at[chunk].reshape(half, width + EXT)
        take = pltpu.make_async_copy(rows_in, xs.at[chunk, pl.ds(0, half)], x_sems.at[chunk])
        take.start()
        forward = pltpu.make_async_remote_copy(
            rows_in, xs.at[chunk, pl.ds(half, half)], fwd_send.at[chunk], fwd_recv.at[chunk],
            device_id=partner, device_id_type=MESH,
        )
        forward.start()
        forwards.append(forward)
        if chunk == 0:
            loads[0].wait()
            loads[1].wait()
        take.wait()
        forward.wait_recv()

        def gate_step(n, carry):
            cols = pl.ds(pl.multiple_of(n * TILE, TILE), TILE)
            block = xs[chunk, :, :width]
            gate = jnp.dot(block, gate_v[:, cols], preferred_element_type=F32)
            up = jnp.dot(block, up_v[:, cols], preferred_element_type=F32)
            hidden[:, cols] = (gate / (1.0 + jnp.exp(-gate)) * up).astype(BF16)
            return carry

        lax.fori_loop(0, w_gate.shape[2] // TILE, gate_step, 0)
        if chunk == 0:
            loads[2].wait()

        def down_to(dest, start):
            def down_step(n, carry):
                cols = pl.ds(pl.multiple_of(n * TILE, TILE), TILE)
                dest[:, cols] = jnp.dot(
                    hidden[start : start + half, :], down_v[:, cols], preferred_element_type=F32
                ).astype(BF16)
                return carry

            lax.fori_loop(0, width // TILE, down_step, 0)

        down_to(theirs.at[chunk], half)
        swap = pltpu.make_async_remote_copy(
            theirs.at[chunk], other.at[chunk], out_send.at[chunk], out_recv.at[chunk],
            device_id=partner, device_id_type=MESH,
        )
        swap.start()
        swaps.append(swap)
        down_to(mine, 0)
        ext = xs[chunk, :half, width:].astype(F32)
        lane = lax.broadcasted_iota(jnp.int32, ext.shape, 1)
        even = jnp.sum(jnp.where(lane < 3, ext, 0.0), axis=1, keepdims=True)
        odd = jnp.sum(jnp.where(lane < 3, 0.0, ext), axis=1, keepdims=True)
        is_even = (jnp.zeros_like(even).astype(jnp.int32) + core) == 0
        w_mine = jnp.where(is_even, even, odd)
        w_other = jnp.where(is_even, odd, even)
        swap.wait_recv()

        def sum_step(n, carry):
            cols = pl.ds(pl.multiple_of(n * TILE, TILE), TILE)
            summed[chunk, :, cols] = (
                w_mine * mine[:, cols].astype(F32) + w_other * other[chunk, :, cols].astype(F32)
            ).astype(BF16)
            return carry

        lax.fori_loop(0, width // TILE, sum_step, 0)
        put = pltpu.make_async_copy(
            summed.at[chunk], pair_out.at[chunk].reshape(half, width), p_sems.at[chunk]
        )
        put.start()
        put.wait()

        def home(q, carry):
            dx, dy, dz = offset_of(chunk, q)
            pltpu.make_async_remote_copy(
                pair_out.at[chunk, q], back.at[chunk, q], back_send.at[chunk], back_recv.at[chunk],
                device_id=device(x + 4 - dx, y + 4 - dy, z + 4 - dz, core), device_id_type=MESH,
            ).start()
            return carry

        lax.fori_loop(first, PER, home, 0)
        if chunk == 0:
            keep = pltpu.make_async_copy(pair_out.at[0, 0], back.at[0, 0], local_sems.at[1])
            keep.start()

    keep.wait()
    for chunk in range(CHUNKS):
        first = 1 if chunk == 0 else 0
        forwards[chunk].wait_send()
        swaps[chunk].wait_send()
        many(send.at[chunk, pl.ds(first, PER - first)], disp_send.at[chunk]).wait()
        many(pair_out.at[chunk, pl.ds(first, PER - first)], back_send.at[chunk]).wait()
        many(back.at[chunk, pl.ds(first, PER - first)], back_recv.at[chunk]).wait()


def mix_body(hot, back, out, rows, sems):
    half = PER * CAP
    copies = []
    for chunk in range(CHUNKS):
        copies.append(
            pltpu.make_async_copy(
                back.at[chunk].reshape(half, out.shape[1]), rows.at[pl.ds(chunk * half, half)],
                sems.at[chunk],
            )
        )
        copies[-1].start()
    for copy in copies:
        copy.wait()
    part = out.shape[1] // 4
    for k in range(4):
        cols = slice(k * part, (k + 1) * part)
        out[:, cols] = jnp.dot(
            hot[...], rows[:, cols], preferred_element_type=F32
        ).astype(out.dtype)


def body(tokens, node_ids, local_ids, affinity, w_gate, w_up, w_down, grad_parts):
    count, width = tokens.shape
    inner = w_gate.shape[2]
    half = PER * CAP
    slots = CHIPS * CAP
    vmem = pl.BlockSpec(memory_space=pltpu.VMEM)
    hbm = pl.BlockSpec(memory_space=pltpu.HBM)
    smem = pl.BlockSpec(memory_space=pltpu.SMEM)
    x, y, z, _ = place()
    pos = jnp.stack([x, y, z]).astype(jnp.int32)
    send, hot = pl.pallas_call(
        prep_body,
        name="prep",
        out_shape=(
            jax.ShapeDtypeStruct((CHUNKS, PER, CAP // 2, 2, width + EXT), BF16),
            jax.ShapeDtypeStruct((count, slots), BF16),
        ),
        in_specs=[smem, vmem, vmem, vmem, vmem],
        out_specs=(hbm, vmem),
        scratch_shapes=[
            pltpu.VMEM((slots, width + EXT), BF16),
            pltpu.SemaphoreType.DMA,
        ],
        compiler_params=pltpu.CompilerParams(vmem_limit_bytes=60 << 20),
    )(pos, node_ids, local_ids, affinity, tokens)

    dma = pltpu.SemaphoreType.DMA
    _, _, back = pl.pallas_call(
        moe_body,
        name="moe",
        out_shape=(
            jax.ShapeDtypeStruct((CHUNKS, PER, CAP // 2, 2, width + EXT), BF16),
            jax.ShapeDtypeStruct((CHUNKS, PER, CAP // 2, 2, width), BF16),
            jax.ShapeDtypeStruct((CHUNKS, PER, CAP // 2, 2, width), BF16),
        ),
        in_specs=[hbm] * 4,
        out_specs=(hbm,) * 3,
        scratch_shapes=[
            pltpu.VMEM((width, inner), BF16),
            pltpu.VMEM((width, inner), BF16),
            pltpu.VMEM((inner, width), BF16),
            pltpu.VMEM((CHUNKS, 2 * half, width + EXT), BF16),
            pltpu.VMEM((2 * half, inner), BF16),
            pltpu.VMEM((CHUNKS, half, width), BF16),
            pltpu.VMEM((half, width), BF16),
            pltpu.VMEM((CHUNKS, half, width), BF16),
            pltpu.VMEM((CHUNKS, half, width), BF16),
            dma((3,)),
            dma((CHUNKS,)), dma((CHUNKS,)), dma((2,)), dma((CHUNKS,)), dma((CHUNKS,)),
            dma((CHUNKS,)), dma((CHUNKS,)), dma((CHUNKS,)), dma((CHUNKS,)), dma((CHUNKS,)),
            dma((CHUNKS,)),
        ],
        compiler_params=pltpu.CompilerParams(
            collective_id=0, has_side_effects=True, vmem_limit_bytes=67043328
        ),
        cost_estimate=pl.CostEstimate(
            flops=6 * 2 * slots * width * inner, bytes_accessed=50 << 20, transcendentals=0
        ),
    )(send, w_gate, w_up, w_down)
    mixed = pl.pallas_call(
        mix_body,
        name="mix",
        out_shape=jax.ShapeDtypeStruct((count, width), BF16),
        in_specs=[vmem, hbm],
        out_specs=vmem,
        scratch_shapes=[pltpu.VMEM((slots, width), BF16), dma((CHUNKS,))],
        compiler_params=pltpu.CompilerParams(vmem_limit_bytes=60 << 20),
    )(hot, back)
    router_grad = lax.psum_scatter(
        grad_parts[0], ("edp", "ep"), scatter_dimension=0, tiled=True
    )
    return mixed, router_grad


def solution(mesh):
    spec2 = P(("edp", "ep"), None)
    spec3 = P(("edp", "ep"), None, None)
    return jax.shard_map(
        body,
        mesh=mesh,
        in_specs=(spec2,) * 4 + (spec3,) * 4,
        out_specs=(spec2, spec2),
        check_vma=False,
    )
```

```python
import jax
import jax.numpy as jnp
from jax import lax
from jax.experimental import pallas as pl
from jax.experimental.pallas import tpu as pltpu
from jax.sharding import PartitionSpec as P

MESH = pl.DeviceIdType.MESH
CHUNKS = 2
CHIPS = 64
PER = CHIPS // CHUNKS
CAP = 10
HALF = PER * CAP
PAIRS = CAP // 2
EXT = 128
TILE = 256
BF16 = jnp.bfloat16
F32 = jnp.float32
I32 = jnp.int32
TURN = (((0,), (0,)), ((), ()))
SIDE = (((1,), (1,)), ((), ()))


def place():
    edp = lax.axis_index("edp")
    ep = lax.axis_index("ep")
    return (ep // 8) % 4, (ep // 2) % 4, (ep // 32) * 2 + edp, ep % 2


def device(x, y, z, core):
    x, y, z = x % 4, y % 4, z % 4
    return {"edp": z % 2, "ep": (z // 2) * 32 + x * 8 + y * 2 + core}


def slot_of(dx, dy, dz):
    return (dx + dy + dz) % CHUNKS, (dx * 4 + dy) * (4 // CHUNKS) + dz // CHUNKS


def send_order():
    far = sorted(
        ((x, y, z) for x in range(4) for y in range(4) for z in range(4)),
        key=lambda o: -sum(min(d, 4 - d) for d in o),
    )
    order = []
    for o in far:
        for k in range(3):
            for s in (1, -1):
                other = tuple(s * o[(i + k) % 3] % 4 for i in range(3))
                if other not in order and any(other):
                    order.append(other)
    return [[o for o in order if slot_of(*o)[0] == chunk] for chunk in range(CHUNKS)]


ORDER = send_order()


def many(ref, sem):
    return pltpu.make_async_copy(ref, ref, sem)


def tile_at(n):
    return pl.ds(pl.multiple_of(n * TILE, TILE), TILE)


def moe_body(
    nodes, locals_, aff, tokens, w_gate, w_up, w_down, grads,
    mixed, router, send, land, pair_out, back,
    node_v, local_v, aff_v, tok_v, gate_v, up_v, down_v, hot, rows, xs, hidden, theirs, mine,
    other, acc, g_mine, g_other, g_sum, g_in, g_tot,
    in_sems, w_sems, row_sems, disp_send, disp_recv, own_sems, fwd_send, fwd_recv, x_sems,
    out_send, out_recv, p_sems, back_send, back_recv, mix_sems,
    g_load, g_swap_send, g_swap_recv, g_send, g_recv, g_out, g_out_send, g_out_recv,
):
    x, y, z, core = place()
    z_lo = lax.axis_index("edp")
    width = tokens.shape[1]
    count = tokens.shape[0]
    partner = {"edp": lax.axis_index("edp"), "ep": lax.axis_index("ep") + 1 - 2 * core}

    small = [
        pltpu.make_async_copy(src, dst, in_sems.at[n])
        for n, (src, dst) in enumerate(
            ((nodes, node_v), (locals_, local_v), (aff, aff_v), (tokens, tok_v))
        )
    ]
    for load in small:
        load.start()
    barrier = pltpu.get_barrier_semaphore()

    def greet(n, carry):
        pl.semaphore_signal(
            barrier, 1, device_id=device(x + n // 16, y + n // 4, z + n, core), device_id_type=MESH
        )
        return carry

    lax.fori_loop(1, CHIPS, greet, 0)
    pl.semaphore_signal(barrier, 1, device_id=partner, device_id_type=MESH)
    g_take = pltpu.make_async_copy(grads.at[core], g_mine, g_load)
    g_take.start()
    loads = [
        pltpu.make_async_copy(w_gate.at[0], gate_v, w_sems.at[0]),
        pltpu.make_async_copy(w_up.at[0], up_v, w_sems.at[1]),
        pltpu.make_async_copy(w_down.at[0], down_v, w_sems.at[2]),
    ]
    for load in loads:
        load.start()
    for load in small:
        load.wait()

    affinity = aff_v[...]
    weight = 2.5 * affinity / jnp.sum(affinity, axis=0, keepdims=True)
    node, local = node_v[...], local_v[...]
    chip_id = lax.broadcasted_iota(I32, (CHIPS, count), 0)
    offsets = []
    hit = jnp.zeros((CHIPS, count), F32)
    for j in range(4):
        pair = node[j : j + 1, :] * 8 + (local[2 * j : 2 * j + 1, :] >> 1)
        pz = ((pair >> 4) & 1) * 2 + (pair >> 5)
        dx = (((pair >> 2) & 3) - x + 4) & 3
        dy = ((pair & 3) - y + 4) & 3
        dz = (pz - z + 4) & 3
        chunk = (dx + dy + dz) & (CHUNKS - 1)
        off = chunk * PER + (dx * 4 + dy) * (4 // CHUNKS) + dz // CHUNKS
        offsets.append(off)
        hit = hit + (chip_id == off).astype(F32)
    row = lax.broadcasted_iota(I32, (count, count), 0)
    col = lax.broadcasted_iota(I32, (count, count), 1)
    earlier = (row < col).astype(F32).astype(BF16)
    before = jnp.dot(hit.astype(BF16), earlier, preferred_element_type=F32)
    slots, pieces = [], []
    for j in range(4):
        rank = jnp.sum(jnp.where(chip_id == offsets[j], before, 0.0), axis=0, keepdims=True)
        slots.append(offsets[j] * CAP + rank.astype(I32))
        lead_even = (local[2 * j : 2 * j + 1, :] & 1) == 0
        first, second = weight[2 * j : 2 * j + 1, :], weight[2 * j + 1 : 2 * j + 2, :]
        parts = jnp.zeros((EXT, count), F32)
        for k, value in enumerate(
            (jnp.where(lead_even, first, second), jnp.where(lead_even, second, first))
        ):
            for part in range(3):
                piece = value.astype(BF16).astype(F32)
                parts = jnp.where(row == 3 * k + part, piece, parts)
                value = value - piece
        pieces.append(parts.astype(BF16))

    def fill(chunk):
        slot_id = lax.broadcasted_iota(I32, (HALF, count), 0) + chunk * HALF
        total = jnp.zeros((HALF, count), F32)
        ext = jnp.zeros((HALF, EXT), F32)
        for j in range(4):
            match = (slot_id == slots[j]).astype(F32)
            total = total + match
            ext = ext + lax.dot_general(
                match.astype(BF16), pieces[j], SIDE, preferred_element_type=F32
            )
        one_hot = total.astype(BF16)
        hot[chunk] = one_hot
        rows[chunk, :, width:] = ext.astype(BF16)
        part = width // 4
        for k in range(4):
            rows[chunk, :, k * part : (k + 1) * part] = jnp.dot(
                one_hot, tok_v[:, k * part : (k + 1) * part], preferred_element_type=F32
            ).astype(BF16)
        copy = pltpu.make_async_copy(
            rows.at[chunk], send.at[chunk].reshape(HALF, width + EXT), row_sems.at[chunk]
        )
        copy.start()
        return copy

    def dispatch(chunk):
        def step(p, carry):
            for o in ORDER[chunk]:
                q = slot_of(*o)[1]
                pltpu.make_async_remote_copy(
                    send.at[chunk, q, p], land.at[chunk, q, p],
                    disp_send.at[chunk], disp_recv.at[chunk],
                    device_id=device(x + o[0], y + o[1], z + o[2], core), device_id_type=MESH,
                ).start()
            return carry

        lax.fori_loop(0, PAIRS, step, 0)

    filled = fill(0)
    pl.semaphore_wait(barrier, CHIPS)
    g_swap = pltpu.make_async_remote_copy(
        grads.at[1 - core], g_other, g_swap_send, g_swap_recv,
        device_id=partner, device_id_type=MESH,
    )
    g_swap.start()
    filled.wait()
    own = pltpu.make_async_copy(send.at[0, 0], land.at[0, 0], own_sems.at[0])
    own.start()
    dispatch(0)
    for chunk in range(1, CHUNKS):
        fill(chunk).wait()
        dispatch(chunk)

    blocks = g_sum.shape[0]
    home_chip = z * 16 + x * 4 + y
    holder = z_lo == core
    g_take.wait()
    g_swap.wait_recv()

    def g_add(k, carry):
        g_sum[k] = (g_mine[k] + g_other[k]).astype(BF16)
        return carry

    lax.fori_loop(0, blocks, g_add, 0)

    def g_push(k, carry):
        tz, tx, ty = (k // 16) * 2 + core, (k // 4) % 4, k % 4
        here = (tz == z) & (tx == x) & (ty == y)

        @pl.when(here)
        def _():
            g_in[home_chip] = g_sum[k]

        @pl.when(jnp.logical_not(here))
        def _():
            pltpu.make_async_remote_copy(
                g_sum.at[k], g_in.at[home_chip], g_send, g_recv,
                device_id=device(tx, ty, tz, core), device_id_type=MESH,
            ).start()

        return carry

    lax.fori_loop(0, blocks, g_push, 0)

    forwards, swaps = [], []
    keep = None
    for chunk in range(CHUNKS):
        first = 1 if chunk == 0 else 0
        if chunk == 0:
            own.wait()
        many(land.at[chunk, pl.ds(first, PER - first)], disp_recv.at[chunk]).wait()
        rows_in = land.at[chunk].reshape(HALF, width + EXT)
        forward = pltpu.make_async_remote_copy(
            rows_in, xs.at[chunk, pl.ds(HALF, HALF)], fwd_send.at[chunk], fwd_recv.at[chunk],
            device_id=partner, device_id_type=MESH,
        )
        forward.start()
        forwards.append(forward)
        take = pltpu.make_async_copy(rows_in, xs.at[chunk, pl.ds(0, HALF)], x_sems.at[chunk])
        take.start()
        if chunk == 0:
            loads[0].wait()
            loads[1].wait()
        take.wait()
        forward.wait_recv()

        def gate_step(n, carry):
            cols = tile_at(n)
            block = xs[chunk, :, :width]
            gate = jnp.dot(block, gate_v[:, cols], preferred_element_type=F32)
            up = jnp.dot(block, up_v[:, cols], preferred_element_type=F32)
            hidden[:, cols] = (gate / (1.0 + jnp.exp(-gate)) * up).astype(BF16)
            return carry

        lax.fori_loop(0, gate_v.shape[1] // TILE, gate_step, 0)
        if chunk == 0:
            loads[2].wait()

        def their_step(n, carry):
            cols = tile_at(n)
            theirs[chunk, :, cols] = jnp.dot(
                hidden[HALF:, :], down_v[:, cols], preferred_element_type=F32
            ).astype(BF16)
            return carry

        lax.fori_loop(0, width // TILE, their_step, 0)
        swap = pltpu.make_async_remote_copy(
            theirs.at[chunk], other.at[chunk], out_send.at[chunk], out_recv.at[chunk],
            device_id=partner, device_id_type=MESH,
        )
        swap.start()
        swaps.append(swap)

        def mine_step(n, carry):
            cols = tile_at(n)
            mine[:, cols] = jnp.dot(
                hidden[:HALF, :], down_v[:, cols], preferred_element_type=F32
            ).astype(BF16)
            return carry

        lax.fori_loop(0, width // TILE, mine_step, 0)
        ext = xs[chunk, :HALF, width:].astype(F32)
        lane = lax.broadcasted_iota(I32, ext.shape, 1)
        even = jnp.sum(jnp.where(lane < 3, ext, 0.0), axis=1, keepdims=True)
        odd = jnp.sum(jnp.where(lane < 3, 0.0, ext), axis=1, keepdims=True)
        is_even = (lax.broadcasted_iota(I32, even.shape, 0) * 0 + core) == 0
        w_mine = jnp.where(is_even, even, odd)
        w_other = jnp.where(is_even, odd, even)
        swap.wait_recv()

        def sum_step(n, carry):
            cols = tile_at(n)
            rows[chunk, :, cols] = (
                w_mine * mine[:, cols].astype(F32) + w_other * other[chunk, :, cols].astype(F32)
            ).astype(BF16)
            return carry

        lax.fori_loop(0, width // TILE, sum_step, 0)
        put = pltpu.make_async_copy(
            rows.at[chunk, :, pl.ds(0, width)], pair_out.at[chunk].reshape(HALF, width),
            p_sems.at[chunk],
        )
        put.start()
        put.wait()

        def home(p, carry):
            for o in ORDER[chunk]:
                q = slot_of(*o)[1]
                pltpu.make_async_remote_copy(
                    pair_out.at[chunk, q, p], back.at[chunk, q, p],
                    back_send.at[chunk], back_recv.at[chunk],
                    device_id=device(x + 4 - o[0], y + 4 - o[1], z + 4 - o[2], core),
                    device_id_type=MESH,
                ).start()
            return carry

        lax.fori_loop(0, PAIRS, home, 0)
        if chunk == 0:
            keep = pltpu.make_async_copy(pair_out.at[0, 0], back.at[0, 0], own_sems.at[1])
            keep.start()

    @pl.when(holder)
    def _():
        many(g_in.at[pl.ds(0, CHIPS - 1)], g_recv).wait()

        def g_fold(s, total):
            return total + g_in[s].astype(F32)

        g_tot[...] = lax.fori_loop(0, CHIPS, g_fold, jnp.zeros(g_tot.shape, F32))

        def g_give(k, carry):
            at = pl.multiple_of(k * 4, 4)
            pltpu.make_async_copy(
                g_tot.at[pl.ds(pl.multiple_of(core * 28 + k * 4, 4), 4)], router.at[pl.ds(at, 4)],
                g_out,
            ).start()
            pltpu.make_async_remote_copy(
                g_tot.at[pl.ds(pl.multiple_of((1 - core) * 28 + k * 4, 4), 4)],
                router.at[pl.ds(at, 4)], g_out_send, g_out_recv,
                device_id=partner, device_id_type=MESH,
            ).start()
            return carry

        lax.fori_loop(0, 7, g_give, 0)

    keep.wait()
    for chunk in range(CHUNKS):
        first = 1 if chunk == 0 else 0
        many(back.at[chunk, pl.ds(first, PER - first)], back_recv.at[chunk]).wait()
        fetch = pltpu.make_async_copy(
            back.at[chunk].reshape(HALF, width), xs.at[chunk, pl.ds(0, HALF), pl.ds(0, width)],
            mix_sems.at[chunk],
        )
        fetch.start()
        fetch.wait()
        part = width // 4
        for k in range(4):
            cols = slice(k * part, (k + 1) * part)
            value = lax.dot_general(
                hot[chunk], xs[chunk, :HALF, cols], TURN, preferred_element_type=F32
            )
            if chunk:
                value = acc[:, cols] + value
            if chunk == CHUNKS - 1:
                mixed[:, cols] = value.astype(BF16)
            else:
                acc[:, cols] = value

    g_swap.wait_send()
    many(g_sum.at[pl.ds(0, blocks - 1)], g_send).wait()

    @pl.when(holder)
    def _():
        many(g_sum.at[0], g_out).wait()
        many(g_sum.at[0], g_out_send).wait()

    @pl.when(jnp.logical_not(holder))
    def _():
        many(g_sum.at[0], g_send).wait()
        many(g_sum.at[0], g_out_recv).wait()

    for chunk in range(CHUNKS):
        first = 1 if chunk == 0 else 0
        forwards[chunk].wait_send()
        swaps[chunk].wait_send()
        many(send.at[chunk, pl.ds(first, PER - first)], disp_send.at[chunk]).wait()
        many(pair_out.at[chunk, pl.ds(first, PER - first)], back_send.at[chunk]).wait()


def body(tokens, node_ids, local_ids, affinity, w_gate, w_up, w_down, grad_parts):
    count, width = tokens.shape
    inner = w_gate.shape[2]
    vmem = pl.BlockSpec(memory_space=pltpu.VMEM)
    hbm = pl.BlockSpec(memory_space=pltpu.HBM)
    dma = pltpu.SemaphoreType.DMA
    per_chunk = dma((CHUNKS,))
    blocks = CHIPS // 2
    deep = grad_parts.shape[1] // CHIPS
    lanes = grad_parts.shape[2]
    wide = jax.ShapeDtypeStruct((CHUNKS, PER, PAIRS, 2, width + EXT), BF16)
    plain = jax.ShapeDtypeStruct((CHUNKS, PER, PAIRS, 2, width), BF16)
    outs = pl.pallas_call(
        moe_body,
        name="moe",
        out_shape=(
            jax.ShapeDtypeStruct((count, width), BF16),
            jax.ShapeDtypeStruct((deep // 2, lanes), F32),
            wide, wide, plain, plain,
        ),
        in_specs=[hbm] * 8,
        out_specs=(vmem,) + (hbm,) * 5,
        scratch_shapes=[
            pltpu.VMEM((4, count), I32),
            pltpu.VMEM((8, count), I32),
            pltpu.VMEM((8, count), F32),
            pltpu.VMEM((count, width), BF16),
            pltpu.VMEM((width, inner), BF16),
            pltpu.VMEM((width, inner), BF16),
            pltpu.VMEM((inner, width), BF16),
            pltpu.VMEM((CHUNKS, HALF, count), BF16),
            pltpu.VMEM((CHUNKS, HALF, width + EXT), BF16),
            pltpu.VMEM((CHUNKS, 2 * HALF, width + EXT), BF16),
            pltpu.VMEM((2 * HALF, inner), BF16),
            pltpu.VMEM((CHUNKS, HALF, width), BF16),
            pltpu.VMEM((HALF, width), BF16),
            pltpu.VMEM((CHUNKS, HALF, width), BF16),
            pltpu.VMEM((count, width), F32),
            pltpu.VMEM((blocks, deep, lanes), F32),
            pltpu.VMEM((blocks, deep, lanes), F32),
            pltpu.VMEM((blocks, deep, lanes), BF16),
            pltpu.VMEM((CHIPS, deep, lanes), BF16),
            pltpu.VMEM((deep, lanes), F32),
            dma((4,)), dma((3,)),
            per_chunk, per_chunk, per_chunk, dma((2,)), per_chunk, per_chunk, per_chunk,
            per_chunk, per_chunk, per_chunk, per_chunk, per_chunk, per_chunk,
            dma, dma, dma, dma, dma, dma, dma, dma,
        ],
        compiler_params=pltpu.CompilerParams(
            collective_id=0, has_side_effects=True, vmem_limit_bytes=67043328
        ),
        cost_estimate=pl.CostEstimate(
            flops=12 * CHIPS * CAP * width * inner, bytes_accessed=50 << 20, transcendentals=0
        ),
    )(
        node_ids.T, local_ids.T, affinity.T, tokens, w_gate, w_up, w_down,
        grad_parts.reshape(2, blocks, deep, lanes),
    )
    return outs[0], outs[1]


def solution(mesh):
    spec2 = P(("edp", "ep"), None)
    spec3 = P(("edp", "ep"), None, None)
    return jax.shard_map(
        body,
        mesh=mesh,
        in_specs=(spec2,) * 4 + (spec3,) * 4,
        out_specs=(spec2, spec2),
        check_vma=False,
    )
```

```python
import jax
import jax.numpy as jnp
from jax import lax
from jax.experimental import pallas as pl
from jax.experimental.pallas import tpu as pltpu
from jax.sharding import PartitionSpec as P

MESH = pl.DeviceIdType.MESH
CHUNKS = 2
HOLD = 0
CHIPS = 64
PER = CHIPS // CHUNKS
CAP = 10
HALF = PER * CAP
PAIRS = CAP // 2
EXT = 128
TILE = 256
WIDE = 512
PARTS = ((0, 2048), (2048, 1536))
BF16 = jnp.bfloat16
F32 = jnp.float32
I32 = jnp.int32
TURN = (((0,), (0,)), ((), ()))
SIDE = (((1,), (1,)), ((), ()))


def place():
    edp = lax.axis_index("edp")
    ep = lax.axis_index("ep")
    return (ep // 8) % 4, (ep // 2) % 4, (ep // 32) * 2 + edp, ep % 2


def device(x, y, z, core):
    x, y, z = x % 4, y % 4, z % 4
    return {"edp": z % 2, "ep": (z // 2) * 32 + x * 8 + y * 2 + core}


def slot_of(dx, dy, dz):
    return (dx + dy + dz) % CHUNKS, (dx * 4 + dy) * (4 // CHUNKS) + dz // CHUNKS


def send_order():
    far = sorted(
        ((x, y, z) for x in range(4) for y in range(4) for z in range(4)),
        key=lambda o: -sum(min(d, 4 - d) for d in o),
    )
    order = []
    for o in far:
        for k in range(3):
            for s in (1, -1):
                other = tuple(s * o[(i + k) % 3] % 4 for i in range(3))
                if other not in order and any(other):
                    order.append(other)
    return [[o for o in order if slot_of(*o)[0] == chunk] for chunk in range(CHUNKS)]


ORDER = send_order()


def many(ref, sem):
    return pltpu.make_async_copy(ref, ref, sem)


def tile_at(n):
    return pl.ds(pl.multiple_of(n * TILE, TILE), TILE)


def moe_body(
    nodes, locals_, aff, tokens, w_gate, w_up, w_down, grads,
    mixed, router, size_in, size_out,
    node_v, local_v, aff_v, tok_v, gate_v, up_v, down_v, hot, rows, xs, hidden, theirs, mine,
    other, back, acc, g_mine, g_other, g_sum, g_in, g_tot,
    in_sems, w_sems, disp_send, disp_recv, fwd_send, fwd_recv,
    out_send, out_recv, back_send, back_recv,
    g_load, g_swap_send, g_swap_recv, g_send, g_recv, g_out, g_out_send, g_out_recv,
):
    x, y, z, core = place()
    z_lo = lax.axis_index("edp")
    width = tokens.shape[1]
    count = tokens.shape[0]
    partner = {"edp": lax.axis_index("edp"), "ep": lax.axis_index("ep") + 1 - 2 * core}

    small = [
        pltpu.make_async_copy(src, dst, in_sems.at[n])
        for n, (src, dst) in enumerate(
            ((nodes, node_v), (locals_, local_v), (aff, aff_v), (tokens, tok_v))
        )
    ]
    for load in small:
        load.start()
    barrier = pltpu.get_barrier_semaphore()

    def greet(n, carry):
        pl.semaphore_signal(
            barrier, 1, device_id=device(x + n // 16, y + n // 4, z + n, core), device_id_type=MESH
        )
        return carry

    lax.fori_loop(1, CHIPS, greet, 0)
    pl.semaphore_signal(barrier, 1, device_id=partner, device_id_type=MESH)
    for load in small:
        load.wait()

    affinity = aff_v[...]
    weight = 2.5 * affinity / jnp.sum(affinity, axis=0, keepdims=True)
    node, local = node_v[...], local_v[...]
    chip_id = lax.broadcasted_iota(I32, (CHIPS, count), 0)
    offsets = []
    hit = jnp.zeros((CHIPS, count), F32)
    for j in range(4):
        pair = node[j : j + 1, :] * 8 + (local[2 * j : 2 * j + 1, :] >> 1)
        pz = ((pair >> 4) & 1) * 2 + (pair >> 5)
        dx = (((pair >> 2) & 3) - x + 4) & 3
        dy = ((pair & 3) - y + 4) & 3
        dz = (pz - z + 4) & 3
        chunk = (dx + dy + dz) & (CHUNKS - 1)
        off = chunk * PER + (dx * 4 + dy) * (4 // CHUNKS) + dz // CHUNKS
        offsets.append(off)
        hit = hit + (chip_id == off).astype(F32)
    row = lax.broadcasted_iota(I32, (count, count), 0)
    col = lax.broadcasted_iota(I32, (count, count), 1)
    earlier = (row < col).astype(F32).astype(BF16)
    before = jnp.dot(hit.astype(BF16), earlier, preferred_element_type=F32)
    slots, pieces = [], []
    for j in range(4):
        rank = jnp.sum(jnp.where(chip_id == offsets[j], before, 0.0), axis=0, keepdims=True)
        slots.append(offsets[j] * CAP + rank.astype(I32))
        lead_even = (local[2 * j : 2 * j + 1, :] & 1) == 0
        first, second = weight[2 * j : 2 * j + 1, :], weight[2 * j + 1 : 2 * j + 2, :]
        parts = jnp.zeros((EXT, count), F32)
        for k, value in enumerate(
            (jnp.where(lead_even, first, second), jnp.where(lead_even, second, first))
        ):
            for part in range(3):
                piece = value.astype(BF16).astype(F32)
                parts = jnp.where(row == 3 * k + part, piece, parts)
                value = value - piece
        pieces.append(parts.astype(BF16))

    def fill(chunk):
        slot_id = lax.broadcasted_iota(I32, (HALF, count), 0) + chunk * HALF
        total = jnp.zeros((HALF, count), F32)
        ext = jnp.zeros((HALF, EXT), F32)
        for j in range(4):
            match = (slot_id == slots[j]).astype(F32)
            total = total + match
            ext = ext + lax.dot_general(
                match.astype(BF16), pieces[j], SIDE, preferred_element_type=F32
            )
        one_hot = total.astype(BF16)
        hot[chunk] = one_hot
        rows[chunk, :, width:] = ext.astype(BF16)
        part = width // 4
        for k in range(4):
            rows[chunk, :, k * part : (k + 1) * part] = jnp.dot(
                one_hot, tok_v[:, k * part : (k + 1) * part], preferred_element_type=F32
            ).astype(BF16)

    def two(ref, chunk, q, p):
        return ref.at[chunk, pl.ds(pl.multiple_of(q * CAP + p * 2, 2), 2)]

    def dispatch(chunk):
        def step(p, carry):
            for o in ORDER[chunk]:
                q = slot_of(*o)[1]
                pltpu.make_async_remote_copy(
                    two(rows, chunk, q, p), two(xs, chunk, q, p),
                    disp_send.at[chunk], disp_recv.at[chunk],
                    device_id=device(x + o[0], y + o[1], z + o[2], core), device_id_type=MESH,
                ).start()
            return carry

        lax.fori_loop(0, PAIRS, step, 0)

    fill(0)
    pl.semaphore_wait(barrier, CHIPS)
    dispatch(0)
    g_take = pltpu.make_async_copy(grads.at[core], g_mine, g_load)
    g_take.start()
    g_swap = pltpu.make_async_remote_copy(
        grads.at[1 - core], g_other, g_swap_send, g_swap_recv,
        device_id=partner, device_id_type=MESH,
    )
    g_swap.start()
    loads = [
        pltpu.make_async_copy(w_gate.at[0], gate_v, w_sems.at[0]),
        pltpu.make_async_copy(w_up.at[0], up_v, w_sems.at[1]),
        pltpu.make_async_copy(w_down.at[0], down_v, w_sems.at[2]),
    ]
    for load in loads:
        load.start()
    for chunk in range(1, CHUNKS):
        fill(chunk)
        dispatch(chunk)
    xs[0, :CAP, :] = rows[0, :CAP, :]

    blocks = g_sum.shape[0]
    home_chip = z * 16 + x * 4 + y
    holder = z_lo == core
    g_take.wait()
    g_swap.wait_recv()

    def g_add(k, carry):
        g_sum[k] = (g_mine[k] + g_other[k]).astype(BF16)
        return carry

    lax.fori_loop(0, blocks, g_add, 0)

    def g_push(k, carry):
        tz, tx, ty = (k // 16) * 2 + core, (k // 4) % 4, k % 4
        here = (tz == z) & (tx == x) & (ty == y)

        @pl.when(here)
        def _():
            g_in[home_chip] = g_sum[k]

        @pl.when(jnp.logical_not(here))
        def _():
            pltpu.make_async_remote_copy(
                g_sum.at[k], g_in.at[home_chip], g_send, g_recv,
                device_id=device(tx, ty, tz, core), device_id_type=MESH,
            ).start()

        return carry

    lax.fori_loop(0, blocks, g_push, 0)

    def dispatched(chunk):
        first = 1 if chunk == 0 else 0
        many(size_in.at[pl.ds(first, PER - first)], disp_send.at[chunk]).wait()

    def go_home(chunk):
        def home(p, carry):
            for o in ORDER[chunk]:
                q = slot_of(*o)[1]
                pltpu.make_async_remote_copy(
                    two(rows.at[:, :, pl.ds(0, width)], chunk, q, p), two(back, chunk, q, p),
                    back_send.at[chunk], back_recv.at[chunk],
                    device_id=device(x + 4 - o[0], y + 4 - o[1], z + 4 - o[2], core),
                    device_id_type=MESH,
                ).start()
            return carry

        lax.fori_loop(0, PAIRS, home, 0)

    forwards, swaps = [], []
    for chunk in range(CHUNKS):
        first = 1 if chunk == 0 else 0
        many(size_in.at[pl.ds(first, PER - first)], disp_recv.at[chunk]).wait()
        forward = pltpu.make_async_remote_copy(
            xs.at[chunk, pl.ds(0, HALF)], xs.at[chunk, pl.ds(HALF, HALF)],
            fwd_send.at[chunk], fwd_recv.at[chunk], device_id=partner, device_id_type=MESH,
        )
        forward.start()
        forwards.append(forward)
        if chunk == 0:
            loads[0].wait()
            loads[1].wait()
        forward.wait_recv()

        for n in range(gate_v.shape[1] // WIDE):
            cols = slice(n * WIDE, (n + 1) * WIDE)
            block = xs[chunk, :, :width]
            gate = jnp.dot(block, gate_v[:, cols], preferred_element_type=F32)
            up = jnp.dot(block, up_v[:, cols], preferred_element_type=F32)
            hidden[:, cols] = (gate / (1.0 + jnp.exp(-gate)) * up).astype(BF16)
        if chunk == 0:
            loads[2].wait()

        for n, (start, size) in enumerate(PARTS):
            cols = slice(start, start + size)
            both = jnp.dot(hidden[...], down_v[:, cols], preferred_element_type=F32).astype(BF16)
            theirs[chunk, :, cols] = both[HALF:]
            mine[:, cols] = both[:HALF]
            swap = pltpu.make_async_remote_copy(
                theirs.at[chunk, :, pl.ds(start, size)], other.at[chunk, :, pl.ds(start, size)],
                out_send.at[chunk, n], out_recv.at[chunk, n],
                device_id=partner, device_id_type=MESH,
            )
            swap.start()
            swaps.append(swap)
        ext = xs[chunk, :HALF, width:].astype(F32)
        lane = lax.broadcasted_iota(I32, ext.shape, 1)
        even = jnp.sum(jnp.where(lane < 3, ext, 0.0), axis=1, keepdims=True)
        odd = jnp.sum(jnp.where(lane < 3, 0.0, ext), axis=1, keepdims=True)
        is_even = (lax.broadcasted_iota(I32, even.shape, 0) * 0 + core) == 0
        w_mine = jnp.where(is_even, even, odd)
        w_other = jnp.where(is_even, odd, even)
        if chunk <= HOLD:
            dispatched(chunk)

        def sum_step(n, carry):
            cols = tile_at(n)
            rows[chunk, :, cols] = (
                w_mine * mine[:, cols].astype(F32) + w_other * other[chunk, :, cols].astype(F32)
            ).astype(BF16)
            return carry

        for n, (start, size) in enumerate(PARTS):
            swaps[chunk * len(PARTS) + n].wait_recv()
            lax.fori_loop(start // TILE, (start + size) // TILE, sum_step, 0)
        if chunk == 0:
            back[0, :CAP, :] = rows[0, :CAP, :width]
        if chunk == HOLD:
            for later in range(chunk + 1, CHUNKS):
                dispatched(later)
        for ready in range(CHUNKS):
            if ready == chunk > HOLD or ready <= chunk == HOLD:
                go_home(ready)

    @pl.when(holder)
    def _():
        many(g_in.at[pl.ds(0, CHIPS - 1)], g_recv).wait()

        def g_fold(s, total):
            return total + g_in[s].astype(F32)

        g_tot[...] = lax.fori_loop(0, CHIPS, g_fold, jnp.zeros(g_tot.shape, F32))

        def g_give(k, carry):
            at = pl.multiple_of(k * 4, 4)
            pltpu.make_async_copy(
                g_tot.at[pl.ds(pl.multiple_of(core * 28 + k * 4, 4), 4)], router.at[pl.ds(at, 4)],
                g_out,
            ).start()
            pltpu.make_async_remote_copy(
                g_tot.at[pl.ds(pl.multiple_of((1 - core) * 28 + k * 4, 4), 4)],
                router.at[pl.ds(at, 4)], g_out_send, g_out_recv,
                device_id=partner, device_id_type=MESH,
            ).start()
            return carry

        lax.fori_loop(0, 7, g_give, 0)

    for chunk in range(CHUNKS):
        first = 1 if chunk == 0 else 0
        many(size_out.at[pl.ds(first, PER - first)], back_recv.at[chunk]).wait()
        part = width // 4
        for k in range(4):
            cols = slice(k * part, (k + 1) * part)
            value = lax.dot_general(
                hot[chunk], back[chunk, :, cols], TURN, preferred_element_type=F32
            )
            if chunk:
                value = acc[:, cols] + value
            if chunk == CHUNKS - 1:
                mixed[:, cols] = value.astype(BF16)
            else:
                acc[:, cols] = value

    g_swap.wait_send()
    many(g_sum.at[pl.ds(0, blocks - 1)], g_send).wait()

    @pl.when(holder)
    def _():
        many(g_sum.at[0], g_out).wait()
        many(g_sum.at[0], g_out_send).wait()

    @pl.when(jnp.logical_not(holder))
    def _():
        many(g_sum.at[0], g_send).wait()
        many(g_sum.at[0], g_out_recv).wait()

    for chunk in range(CHUNKS):
        first = 1 if chunk == 0 else 0
        forwards[chunk].wait_send()
        for n in range(len(PARTS)):
            swaps[chunk * len(PARTS) + n].wait_send()
        many(size_out.at[pl.ds(first, PER - first)], back_send.at[chunk]).wait()


def finish_body(mixed_in, router_in, mixed, router):
    mixed[...] = mixed_in[...]
    router[...] = router_in[...]


def body(tokens, node_ids, local_ids, affinity, w_gate, w_up, w_down, grad_parts):
    count, width = tokens.shape
    inner = w_gate.shape[2]
    vmem = pl.BlockSpec(memory_space=pltpu.VMEM)
    hbm = pl.BlockSpec(memory_space=pltpu.HBM)
    dma = pltpu.SemaphoreType.DMA
    per_chunk = dma((CHUNKS,))
    blocks = CHIPS // 2
    deep = grad_parts.shape[1] // CHIPS
    lanes = grad_parts.shape[2]
    wide = jax.ShapeDtypeStruct((PER, PAIRS, 2, width + EXT), BF16)
    plain = jax.ShapeDtypeStruct((PER, PAIRS, 2, width), BF16)
    outs = pl.pallas_call(
        moe_body,
        name="moe",
        out_shape=(
            jax.ShapeDtypeStruct((count, width), BF16),
            jax.ShapeDtypeStruct((deep // 2, lanes), F32),
            wide, plain,
        ),
        in_specs=[hbm] * 8,
        out_specs=(vmem,) + (hbm,) * 3,
        scratch_shapes=[
            pltpu.VMEM((4, count), I32),
            pltpu.VMEM((8, count), I32),
            pltpu.VMEM((8, count), F32),
            pltpu.VMEM((count, width), BF16),
            pltpu.VMEM((width, inner), BF16),
            pltpu.VMEM((width, inner), BF16),
            pltpu.VMEM((inner, width), BF16),
            pltpu.VMEM((CHUNKS, HALF, count), BF16),
            pltpu.VMEM((CHUNKS, HALF, width + EXT), BF16),
            pltpu.VMEM((CHUNKS, 2 * HALF, width + EXT), BF16),
            pltpu.VMEM((2 * HALF, inner), BF16),
            pltpu.VMEM((CHUNKS, HALF, width), BF16),
            pltpu.VMEM((HALF, width), BF16),
            pltpu.VMEM((CHUNKS, HALF, width), BF16),
            pltpu.VMEM((CHUNKS, HALF, width), BF16),
            pltpu.VMEM((count, width), F32),
            pltpu.VMEM((blocks, deep, lanes), F32),
            pltpu.VMEM((blocks, deep, lanes), F32),
            pltpu.VMEM((blocks, deep, lanes), BF16),
            pltpu.VMEM((CHIPS, deep, lanes), BF16),
            pltpu.VMEM((deep, lanes), F32),
            dma((4,)), dma((3,)),
            per_chunk, per_chunk, per_chunk, per_chunk,
            dma((CHUNKS, len(PARTS))), dma((CHUNKS, len(PARTS))), per_chunk, per_chunk,
            dma, dma, dma, dma, dma, dma, dma, dma,
        ],
        compiler_params=pltpu.CompilerParams(
            collective_id=0, has_side_effects=True, vmem_limit_bytes=67043328
        ),
        cost_estimate=pl.CostEstimate(
            flops=12 * CHIPS * CAP * width * inner, bytes_accessed=50 << 20, transcendentals=0
        ),
    )(
        node_ids.T, local_ids.T, affinity.T, tokens, w_gate, w_up, w_down,
        grad_parts.reshape(2, blocks, deep, lanes),
    )
    return pl.pallas_call(
        finish_body,
        name="finish",
        out_shape=(
            jax.ShapeDtypeStruct((count, width), BF16),
            jax.ShapeDtypeStruct((deep // 2, lanes), F32),
        ),
        in_specs=[vmem, vmem],
        out_specs=(vmem, vmem),
    )(outs[0], outs[1])


def solution(mesh):
    spec2 = P(("edp", "ep"), None)
    spec3 = P(("edp", "ep"), None, None)
    return jax.shard_map(
        body,
        mesh=mesh,
        in_specs=(spec2,) * 4 + (spec3,) * 4,
        out_specs=(spec2, spec2),
        check_vma=False,
    )
```

```python
import jax
import jax.numpy as jnp
from jax import lax
from jax.experimental import pallas as pl
from jax.experimental.pallas import tpu as pltpu
from jax.sharding import PartitionSpec as P

MESH = pl.DeviceIdType.MESH
CHUNKS = 2
HOLD = 0
CHIPS = 64
PER = CHIPS // CHUNKS
CAP = 10
HALF = PER * CAP
PAIRS = CAP // 2
PARTIES = 4 // CHUNKS
TILE = 256
WIDE = 512
PARTS = ((0, 2048), (2048, 1536))
BF16 = jnp.bfloat16
F32 = jnp.float32
I32 = jnp.int32
TURN = (((0,), (0,)), ((), ()))
SIDE = (((1,), (1,)), ((), ()))


def place():
    edp = lax.axis_index("edp")
    ep = lax.axis_index("ep")
    return (ep // 8) % 4, (ep // 2) % 4, (ep // 32) * 2 + edp, ep % 2


def device(x, y, z, core):
    x, y, z = x % 4, y % 4, z % 4
    return {"edp": z % 2, "ep": (z // 2) * 32 + x * 8 + y * 2 + core}


def slot_of(dx, dy, dz):
    kind = (dx + dy + dz) % 4
    return kind % CHUNKS, kind // CHUNKS * 16 + dx * 4 + dy


def send_order():
    far = sorted(
        ((x, y, z) for x in range(4) for y in range(4) for z in range(4)),
        key=lambda o: -sum(min(d, 4 - d) for d in o),
    )
    order = []
    for o in far:
        for k in range(3):
            for s in (1, -1):
                other = tuple(s * o[(i + k) % 3] % 4 for i in range(3))
                if other not in order and any(other):
                    order.append(other)
    return [[o for o in order if slot_of(*o)[0] == chunk] for chunk in range(CHUNKS)]


ORDER = send_order()


def many(ref, sem):
    return pltpu.make_async_copy(ref, ref, sem)


def tile_at(n):
    return pl.ds(pl.multiple_of(n * TILE, TILE), TILE)


def moe_body(
    nodes, locals_, aff, tokens, w_gate, w_up, w_down, grads,
    mixed, router, size_in,
    node_v, local_v, aff_v, tok_v, gate_v, up_v, down_v, hot, rows, xs, hidden, theirs, mine,
    other, back, acc, w_out, w_in, g_mine, g_other, g_sum, g_in, g_tot,
    in_sems, w_sems, disp_send, disp_recv, fwd_send, fwd_recv,
    out_send, out_recv, back_send, back_recv, wt_send, wt_recv,
    g_load, g_swap_send, g_swap_recv, g_send, g_recv, g_out, g_out_send, g_out_recv,
):
    x, y, z, core = place()
    z_lo = lax.axis_index("edp")
    width = tokens.shape[1]
    count = tokens.shape[0]
    partner = {"edp": lax.axis_index("edp"), "ep": lax.axis_index("ep") + 1 - 2 * core}

    small = [
        pltpu.make_async_copy(src, dst, in_sems.at[n])
        for n, (src, dst) in enumerate(
            ((nodes, node_v), (locals_, local_v), (aff, aff_v), (tokens, tok_v))
        )
    ]
    for load in small:
        load.start()
    barrier = pltpu.get_barrier_semaphore()

    def greet(n, carry):
        pl.semaphore_signal(
            barrier, 1, device_id=device(x + n // 16, y + n // 4, z + n, core), device_id_type=MESH
        )
        return carry

    lax.fori_loop(1, CHIPS, greet, 0)
    pl.semaphore_signal(barrier, 1, device_id=partner, device_id_type=MESH)
    for load in small:
        load.wait()

    affinity = aff_v[...]
    weight = 2.5 * affinity / jnp.sum(affinity, axis=0, keepdims=True)
    node, local = node_v[...], local_v[...]
    chip_id = lax.broadcasted_iota(I32, (CHIPS, count), 0)
    offsets = []
    hit = jnp.zeros((CHIPS, count), F32)
    for j in range(4):
        pair = node[j : j + 1, :] * 8 + (local[2 * j : 2 * j + 1, :] >> 1)
        pz = ((pair >> 4) & 1) * 2 + (pair >> 5)
        dx = (((pair >> 2) & 3) - x + 4) & 3
        dy = ((pair & 3) - y + 4) & 3
        dz = (pz - z + 4) & 3
        kind = (dx + dy + dz) & 3
        off = (kind & (CHUNKS - 1)) * PER + (kind // CHUNKS) * 16 + dx * 4 + dy
        offsets.append(off)
        hit = hit + (chip_id == off).astype(F32)
    row = lax.broadcasted_iota(I32, (count, count), 0)
    col = lax.broadcasted_iota(I32, (count, count), 1)
    earlier = (row < col).astype(F32).astype(BF16)
    before = jnp.dot(hit.astype(BF16), earlier, preferred_element_type=F32)
    ranks = [
        jnp.sum(jnp.where(chip_id == offsets[j], before, 0.0), axis=0, keepdims=True).astype(I32)
        for j in range(4)
    ]

    def fill(chunk):
        slot_id = lax.broadcasted_iota(I32, (HALF, count), 0) + chunk * HALF
        total = jnp.zeros((HALF, count), F32)
        for j in range(4):
            total = total + (slot_id == offsets[j] * CAP + ranks[j]).astype(F32)
        one_hot = total.astype(BF16)
        hot[chunk] = one_hot
        part = width // 4
        for k in range(4):
            rows[chunk, :, k * part : (k + 1) * part] = jnp.dot(
                one_hot, tok_v[:, k * part : (k + 1) * part], preferred_element_type=F32
            ).astype(BF16)

    def spread_weights():
        total = jnp.zeros((CHIPS, count), F32)
        for j in range(4):
            lead_even = (local[2 * j : 2 * j + 1, :] & 1) == 0
            first, second = weight[2 * j : 2 * j + 1, :], weight[2 * j + 1 : 2 * j + 2, :]
            match = chip_id == offsets[j]
            for shift, value in (
                (0, jnp.where(lead_even, first, second)),
                (16, jnp.where(lead_even, second, first)),
            ):
                lanes = (row == ranks[j] + shift).astype(F32).astype(BF16)
                for part in range(3):
                    piece = value.astype(BF16).astype(F32)
                    value = value - piece
                    total = total + lax.dot_general(
                        jnp.where(match, piece, 0.0).astype(BF16), lanes, SIDE,
                        preferred_element_type=F32,
                    )
        w_out[...] = total.reshape(CHIPS, 1, count)

    def push_weights():
        for chunk in range(CHUNKS):
            for o in ORDER[chunk]:
                n = chunk * PER + slot_of(*o)[1]
                pltpu.make_async_remote_copy(
                    w_out.at[n], w_in.at[n], wt_send, wt_recv,
                    device_id=device(x + o[0], y + o[1], z + o[2], core), device_id_type=MESH,
                ).start()
        w_in[0] = w_out[0]

    def two(ref, chunk, q, p):
        return ref.at[chunk, pl.ds(pl.multiple_of(q * CAP + p * 2, 2), 2)]

    def dispatch(chunk):
        def step(p, carry):
            for o in ORDER[chunk]:
                q = slot_of(*o)[1]
                pltpu.make_async_remote_copy(
                    two(rows, chunk, q, p), two(xs, chunk, q, p),
                    disp_send.at[chunk], disp_recv.at[chunk],
                    device_id=device(x + o[0], y + o[1], z + o[2], core), device_id_type=MESH,
                ).start()
            return carry

        lax.fori_loop(0, PAIRS, step, 0)

    fill(0)
    pl.semaphore_wait(barrier, CHIPS)
    dispatch(0)
    g_take = pltpu.make_async_copy(grads.at[core], g_mine, g_load)
    g_take.start()
    g_swap = pltpu.make_async_remote_copy(
        grads.at[1 - core], g_other, g_swap_send, g_swap_recv,
        device_id=partner, device_id_type=MESH,
    )
    g_swap.start()
    loads = [
        pltpu.make_async_copy(w_gate.at[0], gate_v, w_sems.at[0]),
        pltpu.make_async_copy(w_up.at[0], up_v, w_sems.at[1]),
        pltpu.make_async_copy(w_down.at[0], down_v, w_sems.at[2]),
    ]
    for load in loads:
        load.start()
    for chunk in range(1, CHUNKS):
        fill(chunk)
        dispatch(chunk)
    xs[0, :CAP] = rows[0, :CAP]
    spread_weights()
    push_weights()

    blocks = g_sum.shape[0]
    home_chip = z * 16 + x * 4 + y
    holder = z_lo == core
    g_take.wait()
    g_swap.wait_recv()

    def g_add(k, carry):
        g_sum[k] = (g_mine[k] + g_other[k]).astype(BF16)
        return carry

    lax.fori_loop(0, blocks, g_add, 0)

    def g_push(k, carry):
        tz, tx, ty = (k // 16) * 2 + core, (k // 4) % 4, k % 4
        here = (tz == z) & (tx == x) & (ty == y)

        @pl.when(here)
        def _():
            g_in[home_chip] = g_sum[k]

        @pl.when(jnp.logical_not(here))
        def _():
            pltpu.make_async_remote_copy(
                g_sum.at[k], g_in.at[home_chip], g_send, g_recv,
                device_id=device(tx, ty, tz, core), device_id_type=MESH,
            ).start()

        return carry

    lax.fori_loop(0, blocks, g_push, 0)

    def dispatched(chunk):
        first = 1 if chunk == 0 else 0
        many(size_in.at[pl.ds(first, PER - first)], disp_send.at[chunk]).wait()

    def go_home(chunk):
        def home(p, carry):
            for o in ORDER[chunk]:
                q = slot_of(*o)[1]
                pltpu.make_async_remote_copy(
                    two(rows, chunk, q, p), two(back, chunk, q, p),
                    back_send.at[chunk, q // 16], back_recv.at[chunk, q // 16],
                    device_id=device(x + 4 - o[0], y + 4 - o[1], z + 4 - o[2], core),
                    device_id_type=MESH,
                ).start()
            return carry

        lax.fori_loop(0, PAIRS, home, 0)

    forwards, swaps = [], []
    for chunk in range(CHUNKS):
        first = 1 if chunk == 0 else 0
        many(size_in.at[pl.ds(first, PER - first)], disp_recv.at[chunk]).wait()
        forward = pltpu.make_async_remote_copy(
            xs.at[chunk, pl.ds(0, HALF)], xs.at[chunk, pl.ds(HALF, HALF)],
            fwd_send.at[chunk], fwd_recv.at[chunk], device_id=partner, device_id_type=MESH,
        )
        forward.start()
        forwards.append(forward)
        if chunk == 0:
            loads[0].wait()
            loads[1].wait()
        forward.wait_recv()

        for n in range(gate_v.shape[1] // WIDE):
            cols = slice(n * WIDE, (n + 1) * WIDE)
            block = xs[chunk]
            gate = jnp.dot(block, gate_v[:, cols], preferred_element_type=F32)
            up = jnp.dot(block, up_v[:, cols], preferred_element_type=F32)
            hidden[:, cols] = (gate / (1.0 + jnp.exp(-gate)) * up).astype(BF16)
        if chunk == 0:
            loads[2].wait()

        for n, (start, size) in enumerate(PARTS):
            cols = slice(start, start + size)
            both = jnp.dot(hidden[...], down_v[:, cols], preferred_element_type=F32).astype(BF16)
            theirs[chunk, :, cols] = both[HALF:]
            mine[:, cols] = both[:HALF]
            swap = pltpu.make_async_remote_copy(
                theirs.at[chunk, :, pl.ds(start, size)], other.at[chunk, :, pl.ds(start, size)],
                out_send.at[chunk, n], out_recv.at[chunk, n],
                device_id=partner, device_id_type=MESH,
            )
            swap.start()
            swaps.append(swap)
        if chunk == 0:
            many(w_in.at[pl.ds(0, CHIPS - 1)], wt_recv).wait()
        spread = w_in[chunk * PER : (chunk + 1) * PER].reshape(PER, count)
        at = lax.broadcasted_iota(I32, (HALF, PER), 0)
        source = (((at * 205) >> 11) == lax.broadcasted_iota(I32, (HALF, PER), 1)).astype(F32)
        table = jnp.zeros((HALF, count), F32)
        for _ in range(3):
            piece = spread.astype(BF16)
            spread = spread - piece.astype(F32)
            table = table + jnp.dot(source.astype(BF16), piece, preferred_element_type=F32)
        at = lax.broadcasted_iota(I32, (HALF, count), 0)
        lane = lax.broadcasted_iota(I32, (HALF, count), 1)
        inside = at - ((at * 205) >> 11) * CAP
        even = jnp.sum(jnp.where(lane == inside, table, 0.0), axis=1, keepdims=True)
        odd = jnp.sum(jnp.where(lane == inside + 16, table, 0.0), axis=1, keepdims=True)
        is_even = (lax.broadcasted_iota(I32, even.shape, 0) * 0 + core) == 0
        w_mine = jnp.where(is_even, even, odd)
        w_other = jnp.where(is_even, odd, even)
        if chunk <= HOLD:
            dispatched(chunk)

        def sum_step(n, carry):
            cols = tile_at(n)
            rows[chunk, :, cols] = (
                w_mine * mine[:, cols].astype(F32) + w_other * other[chunk, :, cols].astype(F32)
            ).astype(BF16)
            return carry

        for n, (start, size) in enumerate(PARTS):
            swaps[chunk * len(PARTS) + n].wait_recv()
            lax.fori_loop(start // TILE, (start + size) // TILE, sum_step, 0)
        if chunk == 0:
            back[0, :CAP] = rows[0, :CAP]
        if chunk == HOLD:
            for later in range(chunk + 1, CHUNKS):
                dispatched(later)
        for ready in range(CHUNKS):
            if ready == chunk > HOLD or ready <= chunk == HOLD:
                go_home(ready)

    @pl.when(holder)
    def _():
        many(g_in.at[pl.ds(0, CHIPS - 1)], g_recv).wait()

        def g_fold(s, total):
            return total + g_in[s].astype(F32)

        g_tot[...] = lax.fori_loop(0, CHIPS, g_fold, jnp.zeros(g_tot.shape, F32))

        def g_give(k, carry):
            at = pl.multiple_of(k * 4, 4)
            pltpu.make_async_copy(
                g_tot.at[pl.ds(pl.multiple_of(core * 28 + k * 4, 4), 4)], router.at[pl.ds(at, 4)],
                g_out,
            ).start()
            pltpu.make_async_remote_copy(
                g_tot.at[pl.ds(pl.multiple_of((1 - core) * 28 + k * 4, 4), 4)],
                router.at[pl.ds(at, 4)], g_out_send, g_out_recv,
                device_id=partner, device_id_type=MESH,
            ).start()
            return carry

        lax.fori_loop(0, 7, g_give, 0)

    for step in range(CHUNKS * PARTIES):
        chunk, party = step // PARTIES, step % PARTIES
        first = 1 if step == 0 else 0
        many(size_in.at[pl.ds(first, 16 - first)], back_recv.at[chunk, party]).wait()
        lot = slice(party * 16 * CAP, (party + 1) * 16 * CAP)
        part = width // 4
        for k in range(4):
            cols = slice(k * part, (k + 1) * part)
            value = lax.dot_general(
                hot[chunk, lot], back[chunk, lot, cols], TURN, preferred_element_type=F32
            )
            if step:
                value = acc[:, cols] + value
            if step == CHUNKS * PARTIES - 1:
                mixed[:, cols] = value.astype(BF16)
            else:
                acc[:, cols] = value

    g_swap.wait_send()
    many(g_sum.at[pl.ds(0, blocks - 1)], g_send).wait()

    @pl.when(holder)
    def _():
        many(g_sum.at[0], g_out).wait()
        many(g_sum.at[0], g_out_send).wait()

    @pl.when(jnp.logical_not(holder))
    def _():
        many(g_sum.at[0], g_send).wait()
        many(g_sum.at[0], g_out_recv).wait()

    many(w_out.at[pl.ds(0, CHIPS - 1)], wt_send).wait()
    for chunk in range(CHUNKS):
        first = 1 if chunk == 0 else 0
        forwards[chunk].wait_send()
        for n in range(len(PARTS)):
            swaps[chunk * len(PARTS) + n].wait_send()
        for party in range(PARTIES):
            skip = first if party == 0 else 0
            many(size_in.at[pl.ds(skip, 16 - skip)], back_send.at[chunk, party]).wait()


def body(tokens, node_ids, local_ids, affinity, w_gate, w_up, w_down, grad_parts):
    count, width = tokens.shape
    inner = w_gate.shape[2]
    vmem = pl.BlockSpec(memory_space=pltpu.VMEM)
    hbm = pl.BlockSpec(memory_space=pltpu.HBM)
    dma = pltpu.SemaphoreType.DMA
    per_chunk = dma((CHUNKS,))
    blocks = CHIPS // 2
    deep = grad_parts.shape[1] // CHIPS
    lanes = grad_parts.shape[2]
    plain = jax.ShapeDtypeStruct((PER, PAIRS, 2, width), BF16)
    outs = pl.pallas_call(
        moe_body,
        name="moe",
        out_shape=(
            pltpu.VMEM((count, width), BF16),
            pltpu.VMEM((deep // 2, lanes), F32),
            plain,
        ),
        in_specs=[hbm] * 8,
        out_specs=(vmem, vmem, hbm),
        scratch_shapes=[
            pltpu.VMEM((4, count), I32),
            pltpu.VMEM((8, count), I32),
            pltpu.VMEM((8, count), F32),
            pltpu.VMEM((count, width), BF16),
            pltpu.VMEM((width, inner), BF16),
            pltpu.VMEM((width, inner), BF16),
            pltpu.VMEM((inner, width), BF16),
            pltpu.VMEM((CHUNKS, HALF, count), BF16),
            pltpu.VMEM((CHUNKS, HALF, width), BF16),
            pltpu.VMEM((CHUNKS, 2 * HALF, width), BF16),
            pltpu.VMEM((2 * HALF, inner), BF16),
            pltpu.VMEM((CHUNKS, HALF, width), BF16),
            pltpu.VMEM((HALF, width), BF16),
            pltpu.VMEM((CHUNKS, HALF, width), BF16),
            pltpu.VMEM((CHUNKS, HALF, width), BF16),
            pltpu.VMEM((count, width), F32),
            pltpu.VMEM((CHIPS, 1, count), F32),
            pltpu.VMEM((CHIPS, 1, count), F32),
            pltpu.VMEM((blocks, deep, lanes), F32),
            pltpu.VMEM((blocks, deep, lanes), F32),
            pltpu.VMEM((blocks, deep, lanes), BF16),
            pltpu.VMEM((CHIPS, deep, lanes), BF16),
            pltpu.VMEM((deep, lanes), F32),
            dma((4,)), dma((3,)),
            per_chunk, per_chunk, per_chunk, per_chunk,
            dma((CHUNKS, len(PARTS))), dma((CHUNKS, len(PARTS))),
            dma((CHUNKS, PARTIES)), dma((CHUNKS, PARTIES)), dma, dma,
            dma, dma, dma, dma, dma, dma, dma, dma,
        ],
        compiler_params=pltpu.CompilerParams(
            collective_id=0, has_side_effects=True, vmem_limit_bytes=64000000
        ),
        cost_estimate=pl.CostEstimate(
            flops=12 * CHIPS * CAP * width * inner, bytes_accessed=50 << 20, transcendentals=0
        ),
    )(
        node_ids.T, local_ids.T, affinity.T, tokens, w_gate, w_up, w_down,
        grad_parts.reshape(2, blocks, deep, lanes),
    )
    return outs[0], outs[1]


def solution(mesh):
    spec2 = P(("edp", "ep"), None)
    spec3 = P(("edp", "ep"), None, None)
    return jax.shard_map(
        body,
        mesh=mesh,
        in_specs=(spec2,) * 4 + (spec3,) * 4,
        out_specs=(spec2, spec2),
        check_vma=False,
    )
```

```python
import jax
import jax.numpy as jnp
from jax import lax
from jax.experimental import pallas as pl
from jax.experimental.pallas import tpu as pltpu
from jax.sharding import PartitionSpec as P

MESH = pl.DeviceIdType.MESH
CHUNKS = 2
HOLD = 0
CHIPS = 64
PER = CHIPS // CHUNKS
CAP = 10
HALF = PER * CAP
PAIRS = CAP // 2
PARTIES = 4 // CHUNKS
TILE = 256
WIDE = 512
PARTS = ((0, 2048), (2048, 1536))
BF16 = jnp.bfloat16
F32 = jnp.float32
I32 = jnp.int32
TURN = (((0,), (0,)), ((), ()))
SIDE = (((1,), (1,)), ((), ()))


def place():
    edp = lax.axis_index("edp")
    ep = lax.axis_index("ep")
    return (ep // 8) % 4, (ep // 2) % 4, (ep // 32) * 2 + edp, ep % 2


def device(x, y, z, core):
    x, y, z = x % 4, y % 4, z % 4
    return {"edp": z % 2, "ep": (z // 2) * 32 + x * 8 + y * 2 + core}


def slot_of(dx, dy, dz):
    kind = (dx + dy + dz) % 4
    return kind % CHUNKS, kind // CHUNKS * 16 + dx * 4 + dy


def send_order():
    far = sorted(
        ((x, y, z) for x in range(4) for y in range(4) for z in range(4)),
        key=lambda o: -sum(min(d, 4 - d) for d in o),
    )
    order = []
    for o in far:
        for k in range(3):
            for s in (1, -1):
                other = tuple(s * o[(i + k) % 3] % 4 for i in range(3))
                if other not in order and any(other):
                    order.append(other)
    return [[o for o in order if slot_of(*o)[0] == chunk] for chunk in range(CHUNKS)]


ORDER = send_order()


def many(ref, sem):
    return pltpu.make_async_copy(ref, ref, sem)


def tile_at(n):
    return pl.ds(pl.multiple_of(n * TILE, TILE), TILE)


def moe_body(
    nodes, locals_, aff, tokens, w_gate, w_up, w_down, grads,
    mixed, router, size_in,
    node_v, local_v, aff_v, tok_v, gate_v, up_v, down_v, hot, rows, xs, hidden, theirs, mine,
    other, back, acc, w_out, w_in, g_mine, g_other, g_sum, g_in, g_tot,
    in_sems, w_sems, disp_send, disp_recv, fwd_send, fwd_recv,
    out_send, out_recv, back_send, back_recv, wt_send, wt_recv,
    g_load, g_swap_send, g_swap_recv, g_send, g_recv, g_out, g_out_send, g_out_recv,
):
    x, y, z, core = place()
    z_lo = lax.axis_index("edp")
    width = tokens.shape[1]
    count = tokens.shape[0]
    partner = {"edp": lax.axis_index("edp"), "ep": lax.axis_index("ep") + 1 - 2 * core}

    small = [
        pltpu.make_async_copy(src, dst, in_sems.at[n])
        for n, (src, dst) in enumerate(
            ((nodes, node_v), (locals_, local_v), (aff, aff_v), (tokens, tok_v))
        )
    ]
    for load in small:
        load.start()
    barrier = pltpu.get_barrier_semaphore()

    along_x = [(x + d) % 4 * 8 for d in range(4)]
    along_y = [(y + d) % 4 * 2 + core for d in range(4)]
    along_z = [(z + d) % 4 // 2 * 32 for d in range(4)]
    halves = [(z + d) % 2 for d in range(2)]

    def peer(o, sign=1):
        dx, dy, dz = (sign * d % 4 for d in o)
        return {"edp": halves[dz % 2], "ep": along_z[dz] + along_x[dx] + along_y[dy]}

    for o in sorted(ORDER[0] + ORDER[1], key=lambda o: -sum(min(d, 4 - d) for d in o)):
        pl.semaphore_signal(barrier, 1, device_id=peer(o), device_id_type=MESH)
    pl.semaphore_signal(barrier, 1, device_id=partner, device_id_type=MESH)
    for load in small:
        load.wait()

    affinity = aff_v[...]
    weight = 2.5 * affinity / jnp.sum(affinity, axis=0, keepdims=True)
    node, local = node_v[...], local_v[...]
    chip_id = lax.broadcasted_iota(I32, (CHIPS, count), 0)
    offsets = []
    hit = jnp.zeros((CHIPS, count), F32)
    for j in range(4):
        pair = node[j : j + 1, :] * 8 + (local[2 * j : 2 * j + 1, :] >> 1)
        pz = ((pair >> 4) & 1) * 2 + (pair >> 5)
        dx = (((pair >> 2) & 3) - x + 4) & 3
        dy = ((pair & 3) - y + 4) & 3
        dz = (pz - z + 4) & 3
        kind = (dx + dy + dz) & 3
        off = (kind & (CHUNKS - 1)) * PER + (kind // CHUNKS) * 16 + dx * 4 + dy
        offsets.append(off)
        hit = hit + (chip_id == off).astype(F32)
    row = lax.broadcasted_iota(I32, (count, count), 0)
    col = lax.broadcasted_iota(I32, (count, count), 1)
    earlier = (row < col).astype(F32).astype(BF16)
    before = jnp.dot(hit.astype(BF16), earlier, preferred_element_type=F32)
    ranks = [
        jnp.sum(jnp.where(chip_id == offsets[j], before, 0.0), axis=0, keepdims=True).astype(I32)
        for j in range(4)
    ]

    def fill(chunk):
        slot_id = lax.broadcasted_iota(I32, (HALF, count), 0) + chunk * HALF
        total = jnp.zeros((HALF, count), F32)
        for j in range(4):
            total = total + (slot_id == offsets[j] * CAP + ranks[j]).astype(F32)
        one_hot = total.astype(BF16)
        hot[chunk] = one_hot
        part = width // 4
        for k in range(4):
            rows[chunk, :, k * part : (k + 1) * part] = jnp.dot(
                one_hot, tok_v[:, k * part : (k + 1) * part], preferred_element_type=F32
            ).astype(BF16)

    def spread_weights():
        total = jnp.zeros((CHIPS, count), F32)
        for j in range(4):
            lead_even = (local[2 * j : 2 * j + 1, :] & 1) == 0
            first, second = weight[2 * j : 2 * j + 1, :], weight[2 * j + 1 : 2 * j + 2, :]
            match = chip_id == offsets[j]
            for shift, value in (
                (0, jnp.where(lead_even, first, second)),
                (16, jnp.where(lead_even, second, first)),
            ):
                lanes = (row == ranks[j] + shift).astype(F32).astype(BF16)
                for part in range(3):
                    piece = value.astype(BF16).astype(F32)
                    value = value - piece
                    total = total + lax.dot_general(
                        jnp.where(match, piece, 0.0).astype(BF16), lanes, SIDE,
                        preferred_element_type=F32,
                    )
        w_out[...] = total.reshape(CHIPS, 1, count)

    def push_weights():
        for chunk in range(CHUNKS):
            for o in ORDER[chunk]:
                n = chunk * PER + slot_of(*o)[1]
                pltpu.make_async_remote_copy(
                    w_out.at[n], w_in.at[n], wt_send, wt_recv,
                    device_id=peer(o), device_id_type=MESH,
                ).start()
        w_in[0] = w_out[0]

    def two(ref, chunk, q, p):
        return ref.at[chunk, pl.ds(pl.multiple_of(q * CAP + p * 2, 2), 2)]

    def dispatch(chunk):
        def step(p, carry):
            for o in ORDER[chunk]:
                q = slot_of(*o)[1]
                pltpu.make_async_remote_copy(
                    two(rows, chunk, q, p), two(xs, chunk, q, p),
                    disp_send.at[chunk], disp_recv.at[chunk],
                    device_id=peer(o), device_id_type=MESH,
                ).start()
            return carry

        lax.fori_loop(0, PAIRS, step, 0)

    fill(0)
    pl.semaphore_wait(barrier, CHIPS)
    dispatch(0)
    g_take = pltpu.make_async_copy(grads.at[core], g_mine, g_load)
    g_take.start()
    g_swap = pltpu.make_async_remote_copy(
        grads.at[1 - core], g_other, g_swap_send, g_swap_recv,
        device_id=partner, device_id_type=MESH,
    )
    g_swap.start()
    loads = [
        pltpu.make_async_copy(w_gate.at[0], gate_v, w_sems.at[0]),
        pltpu.make_async_copy(w_up.at[0], up_v, w_sems.at[1]),
        pltpu.make_async_copy(w_down.at[0], down_v, w_sems.at[2]),
    ]
    for load in loads:
        load.start()
    for chunk in range(1, CHUNKS):
        fill(chunk)
        dispatch(chunk)
    xs[0, :CAP] = rows[0, :CAP]
    spread_weights()
    push_weights()

    blocks = g_sum.shape[0]
    home_chip = z * 16 + x * 4 + y
    holder = z_lo == core
    g_take.wait()
    g_swap.wait_recv()

    def g_add(k, carry):
        g_sum[k] = (g_mine[k] + g_other[k]).astype(BF16)
        return carry

    lax.fori_loop(0, blocks, g_add, 0)

    def g_push(k, carry):
        tz, tx, ty = (k // 16) * 2 + core, (k // 4) % 4, k % 4
        here = (tz == z) & (tx == x) & (ty == y)

        @pl.when(here)
        def _():
            g_in[home_chip] = g_sum[k]

        @pl.when(jnp.logical_not(here))
        def _():
            pltpu.make_async_remote_copy(
                g_sum.at[k], g_in.at[home_chip], g_send, g_recv,
                device_id=device(tx, ty, tz, core), device_id_type=MESH,
            ).start()

        return carry

    lax.fori_loop(0, blocks, g_push, 0)

    def dispatched(chunk):
        first = 1 if chunk == 0 else 0
        many(size_in.at[pl.ds(first, PER - first)], disp_send.at[chunk]).wait()

    def go_home(chunk):
        def home(p, carry):
            for o in ORDER[chunk]:
                q = slot_of(*o)[1]
                pltpu.make_async_remote_copy(
                    two(rows, chunk, q, p), two(back, chunk, q, p),
                    back_send.at[chunk, q // 16], back_recv.at[chunk, q // 16],
                    device_id=peer(o, -1),
                    device_id_type=MESH,
                ).start()
            return carry

        lax.fori_loop(0, PAIRS, home, 0)

    forwards, swaps = [], []

    def pass_on(chunk):
        first = 1 if chunk == 0 else 0
        many(size_in.at[pl.ds(first, PER - first)], disp_recv.at[chunk]).wait()
        forward = pltpu.make_async_remote_copy(
            xs.at[chunk, pl.ds(0, HALF)], xs.at[chunk, pl.ds(HALF, HALF)],
            fwd_send.at[chunk], fwd_recv.at[chunk], device_id=partner, device_id_type=MESH,
        )
        forward.start()
        forwards.append(forward)

    for chunk in range(CHUNKS):
        if chunk == 0:
            pass_on(0)
        forward = forwards[chunk]
        if chunk == 0:
            loads[0].wait()
            loads[1].wait()
        forward.wait_recv()

        for n in range(gate_v.shape[1] // WIDE):
            cols = slice(n * WIDE, (n + 1) * WIDE)
            block = xs[chunk]
            gate = jnp.dot(block, gate_v[:, cols], preferred_element_type=F32)
            up = jnp.dot(block, up_v[:, cols], preferred_element_type=F32)
            hidden[:, cols] = (gate / (1.0 + jnp.exp(-gate)) * up).astype(BF16)
        if chunk == 0:
            loads[2].wait()

        for n, (start, size) in enumerate(PARTS):
            cols = slice(start, start + size)
            both = jnp.dot(hidden[...], down_v[:, cols], preferred_element_type=F32).astype(BF16)
            theirs[chunk, :, cols] = both[HALF:]
            mine[:, cols] = both[:HALF]
            swap = pltpu.make_async_remote_copy(
                theirs.at[chunk, :, pl.ds(start, size)], other.at[chunk, :, pl.ds(start, size)],
                out_send.at[chunk, n], out_recv.at[chunk, n],
                device_id=partner, device_id_type=MESH,
            )
            swap.start()
            swaps.append(swap)
        if chunk == 0:
            many(w_in.at[pl.ds(0, CHIPS - 1)], wt_recv).wait()
        spread = w_in[chunk * PER : (chunk + 1) * PER].reshape(PER, count)
        at = lax.broadcasted_iota(I32, (HALF, PER), 0)
        source = (((at * 205) >> 11) == lax.broadcasted_iota(I32, (HALF, PER), 1)).astype(F32)
        table = jnp.zeros((HALF, count), F32)
        for _ in range(3):
            piece = spread.astype(BF16)
            spread = spread - piece.astype(F32)
            table = table + jnp.dot(source.astype(BF16), piece, preferred_element_type=F32)
        at = lax.broadcasted_iota(I32, (HALF, count), 0)
        lane = lax.broadcasted_iota(I32, (HALF, count), 1)
        inside = at - ((at * 205) >> 11) * CAP
        even = jnp.sum(jnp.where(lane == inside, table, 0.0), axis=1, keepdims=True)
        odd = jnp.sum(jnp.where(lane == inside + 16, table, 0.0), axis=1, keepdims=True)
        is_even = (lax.broadcasted_iota(I32, even.shape, 0) * 0 + core) == 0
        w_mine = jnp.where(is_even, even, odd)
        w_other = jnp.where(is_even, odd, even)
        if chunk <= HOLD:
            dispatched(chunk)

        def sum_step(n, carry):
            cols = tile_at(n)
            rows[chunk, :, cols] = (
                w_mine * mine[:, cols].astype(F32) + w_other * other[chunk, :, cols].astype(F32)
            ).astype(BF16)
            return carry

        for n, (start, size) in enumerate(PARTS):
            swaps[chunk * len(PARTS) + n].wait_recv()
            lax.fori_loop(start // TILE, (start + size) // TILE, sum_step, 0)
        if chunk == 0:
            back[0, :CAP] = rows[0, :CAP]
        if chunk == HOLD:
            for later in range(chunk + 1, CHUNKS):
                dispatched(later)
        if chunk + 1 < CHUNKS:
            pass_on(chunk + 1)
        for ready in range(CHUNKS):
            if ready == chunk > HOLD or ready <= chunk == HOLD:
                go_home(ready)

    @pl.when(holder)
    def _():
        many(g_in.at[pl.ds(0, CHIPS - 1)], g_recv).wait()

        def g_fold(s, total):
            return total + g_in[s].astype(F32)

        g_tot[...] = lax.fori_loop(0, CHIPS, g_fold, jnp.zeros(g_tot.shape, F32))

        def g_give(k, carry):
            at = pl.multiple_of(k * 4, 4)
            pltpu.make_async_copy(
                g_tot.at[pl.ds(pl.multiple_of(core * 28 + k * 4, 4), 4)], router.at[pl.ds(at, 4)],
                g_out,
            ).start()
            pltpu.make_async_remote_copy(
                g_tot.at[pl.ds(pl.multiple_of((1 - core) * 28 + k * 4, 4), 4)],
                router.at[pl.ds(at, 4)], g_out_send, g_out_recv,
                device_id=partner, device_id_type=MESH,
            ).start()
            return carry

        lax.fori_loop(0, 7, g_give, 0)

    for step in range(CHUNKS * PARTIES):
        chunk, party = step // PARTIES, step % PARTIES
        first = 1 if step == 0 else 0
        many(size_in.at[pl.ds(first, 16 - first)], back_recv.at[chunk, party]).wait()
        lot = slice(party * 16 * CAP, (party + 1) * 16 * CAP)
        part = width // 4
        for k in range(4):
            cols = slice(k * part, (k + 1) * part)
            value = lax.dot_general(
                hot[chunk, lot], back[chunk, lot, cols], TURN, preferred_element_type=F32
            )
            if step:
                value = acc[:, cols] + value
            if step == CHUNKS * PARTIES - 1:
                mixed[:, cols] = value.astype(BF16)
            else:
                acc[:, cols] = value

    g_swap.wait_send()
    many(g_sum.at[pl.ds(0, blocks - 1)], g_send).wait()

    @pl.when(holder)
    def _():
        many(g_sum.at[0], g_out).wait()
        many(g_sum.at[0], g_out_send).wait()

    @pl.when(jnp.logical_not(holder))
    def _():
        many(g_sum.at[0], g_send).wait()
        many(g_sum.at[0], g_out_recv).wait()

    many(w_out.at[pl.ds(0, CHIPS - 1)], wt_send).wait()
    for chunk in range(CHUNKS):
        first = 1 if chunk == 0 else 0
        forwards[chunk].wait_send()
        for n in range(len(PARTS)):
            swaps[chunk * len(PARTS) + n].wait_send()
        for party in range(PARTIES):
            skip = first if party == 0 else 0
            many(size_in.at[pl.ds(skip, 16 - skip)], back_send.at[chunk, party]).wait()


def body(tokens, node_ids, local_ids, affinity, w_gate, w_up, w_down, grad_parts):
    count, width = tokens.shape
    inner = w_gate.shape[2]
    vmem = pl.BlockSpec(memory_space=pltpu.VMEM)
    hbm = pl.BlockSpec(memory_space=pltpu.HBM)
    dma = pltpu.SemaphoreType.DMA
    per_chunk = dma((CHUNKS,))
    blocks = CHIPS // 2
    deep = grad_parts.shape[1] // CHIPS
    lanes = grad_parts.shape[2]
    plain = jax.ShapeDtypeStruct((PER, PAIRS, 2, width), BF16)
    outs = pl.pallas_call(
        moe_body,
        name="moe",
        out_shape=(
            pltpu.VMEM((count, width), BF16),
            pltpu.VMEM((deep // 2, lanes), F32),
            plain,
        ),
        in_specs=[hbm] * 8,
        out_specs=(vmem, vmem, hbm),
        scratch_shapes=[
            pltpu.VMEM((4, count), I32),
            pltpu.VMEM((8, count), I32),
            pltpu.VMEM((8, count), F32),
            pltpu.VMEM((count, width), BF16),
            pltpu.VMEM((width, inner), BF16),
            pltpu.VMEM((width, inner), BF16),
            pltpu.VMEM((inner, width), BF16),
            pltpu.VMEM((CHUNKS, HALF, count), BF16),
            pltpu.VMEM((CHUNKS, HALF, width), BF16),
            pltpu.VMEM((CHUNKS, 2 * HALF, width), BF16),
            pltpu.VMEM((2 * HALF, inner), BF16),
            pltpu.VMEM((CHUNKS, HALF, width), BF16),
            pltpu.VMEM((HALF, width), BF16),
            pltpu.VMEM((CHUNKS, HALF, width), BF16),
            pltpu.VMEM((CHUNKS, HALF, width), BF16),
            pltpu.VMEM((count, width), F32),
            pltpu.VMEM((CHIPS, 1, count), F32),
            pltpu.VMEM((CHIPS, 1, count), F32),
            pltpu.VMEM((blocks, deep, lanes), F32),
            pltpu.VMEM((blocks, deep, lanes), F32),
            pltpu.VMEM((blocks, deep, lanes), BF16),
            pltpu.VMEM((CHIPS, deep, lanes), BF16),
            pltpu.VMEM((deep, lanes), F32),
            dma((4,)), dma((3,)),
            per_chunk, per_chunk, per_chunk, per_chunk,
            dma((CHUNKS, len(PARTS))), dma((CHUNKS, len(PARTS))),
            dma((CHUNKS, PARTIES)), dma((CHUNKS, PARTIES)), dma, dma,
            dma, dma, dma, dma, dma, dma, dma, dma,
        ],
        compiler_params=pltpu.CompilerParams(
            collective_id=0, has_side_effects=True, vmem_limit_bytes=64000000
        ),
        cost_estimate=pl.CostEstimate(
            flops=12 * CHIPS * CAP * width * inner, bytes_accessed=50 << 20, transcendentals=0
        ),
    )(
        node_ids.T, local_ids.T, affinity.T, tokens, w_gate, w_up, w_down,
        grad_parts.reshape(2, blocks, deep, lanes),
    )
    return outs[0], outs[1]


def solution(mesh):
    spec2 = P(("edp", "ep"), None)
    spec3 = P(("edp", "ep"), None, None)
    return jax.shard_map(
        body,
        mesh=mesh,
        in_specs=(spec2,) * 4 + (spec3,) * 4,
        out_specs=(spec2, spec2),
        check_vma=False,
    )
```

```python
import jax
import jax.numpy as jnp
from jax import lax
from jax.experimental import pallas as pl
from jax.experimental.pallas import tpu as pltpu
from jax.sharding import PartitionSpec as P

MESH = pl.DeviceIdType.MESH
CHUNKS = 2
HOLD = 0
CHIPS = 64
PER = CHIPS // CHUNKS
CAP = 10
HALF = PER * CAP
PAIRS = CAP // 2
PARTIES = 4 // CHUNKS
TILE = 256
WIDE = 512
PARTS = ((0, 2048), (2048, 1536))
BF16 = jnp.bfloat16
F32 = jnp.float32
I32 = jnp.int32
TURN = (((0,), (0,)), ((), ()))
SIDE = (((1,), (1,)), ((), ()))


def place():
    edp = lax.axis_index("edp")
    ep = lax.axis_index("ep")
    return (ep // 8) % 4, (ep // 2) % 4, (ep // 32) * 2 + edp, ep % 2


def device(x, y, z, core):
    x, y, z = x % 4, y % 4, z % 4
    return {"edp": z % 2, "ep": (z // 2) * 32 + x * 8 + y * 2 + core}


def slot_of(dx, dy, dz):
    kind = (dx + dy + dz) % 4
    return kind % CHUNKS, kind // CHUNKS * 16 + dx * 4 + dy


def send_order():
    far = sorted(
        ((x, y, z) for x in range(4) for y in range(4) for z in range(4)),
        key=lambda o: -sum(min(d, 4 - d) for d in o),
    )
    order = []
    for o in far:
        for k in range(3):
            for s in (1, -1):
                other = tuple(s * o[(i + k) % 3] % 4 for i in range(3))
                if other not in order and any(other):
                    order.append(other)
    return [[o for o in order if slot_of(*o)[0] == chunk] for chunk in range(CHUNKS)]


ORDER = send_order()


def many(ref, sem):
    return pltpu.make_async_copy(ref, ref, sem)


def tile_at(n):
    return pl.ds(pl.multiple_of(n * TILE, TILE), TILE)


def moe_body(
    nodes, locals_, aff, tokens, w_gate, w_up, w_down, grads,
    mixed, router, size_in,
    node_v, local_v, aff_v, tok_v, gate_v, up_v, down_v, hot, rows, xs, hidden, theirs, mine,
    other, back, acc, w_out, w_in, g_mine, g_other, g_sum, g_in, g_tot,
    in_sems, w_sems, disp_send, disp_recv, fwd_send, fwd_recv,
    out_send, out_recv, back_send, back_recv, wt_send, wt_recv,
    g_load, g_swap_send, g_swap_recv, g_send, g_recv, g_out, g_out_send, g_out_recv,
):
    x, y, z, core = place()
    z_lo = lax.axis_index("edp")
    width = tokens.shape[1]
    count = tokens.shape[0]
    partner = {"edp": lax.axis_index("edp"), "ep": lax.axis_index("ep") + 1 - 2 * core}

    small = [
        pltpu.make_async_copy(src, dst, in_sems.at[n])
        for n, (src, dst) in enumerate(
            ((nodes, node_v), (locals_, local_v), (aff, aff_v), (tokens, tok_v))
        )
    ]
    for load in small:
        load.start()
    barrier = pltpu.get_barrier_semaphore()

    along_x = [(x + d) % 4 * 8 for d in range(4)]
    along_y = [(y + d) % 4 * 2 + core for d in range(4)]
    along_z = [(z + d) % 4 // 2 * 32 for d in range(4)]
    halves = [(z + d) % 2 for d in range(2)]

    def peer(o, sign=1):
        dx, dy, dz = (sign * d % 4 for d in o)
        return {"edp": halves[dz % 2], "ep": along_z[dz] + along_x[dx] + along_y[dy]}

    for o in sorted(ORDER[0] + ORDER[1], key=lambda o: -sum(min(d, 4 - d) for d in o)):
        pl.semaphore_signal(barrier, 1, device_id=peer(o), device_id_type=MESH)
    pl.semaphore_signal(barrier, 1, device_id=partner, device_id_type=MESH)
    for load in small[:3]:
        load.wait()

    affinity = aff_v[...]
    weight = 2.5 * affinity / jnp.sum(affinity, axis=0, keepdims=True)
    node, local = node_v[...], local_v[...]
    chip_id = lax.broadcasted_iota(I32, (CHIPS, count), 0)
    offsets = []
    hit = jnp.zeros((CHIPS, count), F32)
    for j in range(4):
        pair = node[j : j + 1, :] * 8 + (local[2 * j : 2 * j + 1, :] >> 1)
        pz = ((pair >> 4) & 1) * 2 + (pair >> 5)
        dx = (((pair >> 2) & 3) - x + 4) & 3
        dy = ((pair & 3) - y + 4) & 3
        dz = (pz - z + 4) & 3
        kind = (dx + dy + dz) & 3
        off = (kind & (CHUNKS - 1)) * PER + (kind // CHUNKS) * 16 + dx * 4 + dy
        offsets.append(off)
        hit = hit + (chip_id == off).astype(F32)
    row = lax.broadcasted_iota(I32, (count, count), 0)
    col = lax.broadcasted_iota(I32, (count, count), 1)
    earlier = (row < col).astype(F32).astype(BF16)
    before = jnp.dot(hit.astype(BF16), earlier, preferred_element_type=F32)
    ranks = [
        jnp.sum(jnp.where(chip_id == offsets[j], before, 0.0), axis=0, keepdims=True).astype(I32)
        for j in range(4)
    ]

    def fill(chunk):
        slot_id = lax.broadcasted_iota(I32, (HALF, count), 0) + chunk * HALF
        total = jnp.zeros((HALF, count), F32)
        for j in range(4):
            total = total + (slot_id == offsets[j] * CAP + ranks[j]).astype(F32)
        one_hot = total.astype(BF16)
        hot[chunk] = one_hot
        part = width // 4
        for k in range(4):
            rows[chunk, :, k * part : (k + 1) * part] = jnp.dot(
                one_hot, tok_v[:, k * part : (k + 1) * part], preferred_element_type=F32
            ).astype(BF16)

    def spread_weights():
        total = jnp.zeros((CHIPS, count), F32)
        for j in range(4):
            lead_even = (local[2 * j : 2 * j + 1, :] & 1) == 0
            first, second = weight[2 * j : 2 * j + 1, :], weight[2 * j + 1 : 2 * j + 2, :]
            match = chip_id == offsets[j]
            for shift, value in (
                (0, jnp.where(lead_even, first, second)),
                (16, jnp.where(lead_even, second, first)),
            ):
                lanes = (row == ranks[j] + shift).astype(F32).astype(BF16)
                for part in range(3):
                    piece = value.astype(BF16).astype(F32)
                    value = value - piece
                    total = total + lax.dot_general(
                        jnp.where(match, piece, 0.0).astype(BF16), lanes, SIDE,
                        preferred_element_type=F32,
                    )
        w_out[...] = total.reshape(CHIPS, 1, count)

    def push_weights():
        for chunk in range(CHUNKS):
            for o in ORDER[chunk]:
                n = chunk * PER + slot_of(*o)[1]
                pltpu.make_async_remote_copy(
                    w_out.at[n], w_in.at[n], wt_send, wt_recv,
                    device_id=peer(o), device_id_type=MESH,
                ).start()
        w_in[0] = w_out[0]

    def two(ref, chunk, q, p):
        return ref.at[chunk, pl.ds(pl.multiple_of(q * CAP + p * 2, 2), 2)]

    def dispatch(chunk):
        def step(p, carry):
            for o in ORDER[chunk]:
                q = slot_of(*o)[1]
                pltpu.make_async_remote_copy(
                    two(rows, chunk, q, p), two(xs, chunk, q, p),
                    disp_send.at[chunk], disp_recv.at[chunk],
                    device_id=peer(o), device_id_type=MESH,
                ).start()
            return carry

        lax.fori_loop(0, PAIRS, step, 0)

    small[3].wait()
    fill(0)
    pl.semaphore_wait(barrier, CHIPS)
    dispatch(0)
    g_take = pltpu.make_async_copy(grads.at[core], g_mine, g_load)
    g_take.start()
    g_swap = pltpu.make_async_remote_copy(
        grads.at[1 - core], g_other, g_swap_send, g_swap_recv,
        device_id=partner, device_id_type=MESH,
    )
    g_swap.start()
    loads = [
        pltpu.make_async_copy(w_gate.at[0], gate_v, w_sems.at[0]),
        pltpu.make_async_copy(w_up.at[0], up_v, w_sems.at[1]),
        pltpu.make_async_copy(w_down.at[0], down_v, w_sems.at[2]),
    ]
    for load in loads:
        load.start()
    for chunk in range(1, CHUNKS):
        fill(chunk)
        dispatch(chunk)
    xs[0, :CAP] = rows[0, :CAP]
    spread_weights()
    push_weights()

    blocks = g_sum.shape[0]
    home_chip = z * 16 + x * 4 + y
    holder = z_lo == core
    g_take.wait()
    g_swap.wait_recv()

    def g_add(k, carry):
        g_sum[k] = (g_mine[k] + g_other[k]).astype(BF16)
        return carry

    lax.fori_loop(0, blocks, g_add, 0)

    def g_push(k, carry):
        tz, tx, ty = (k // 16) * 2 + core, (k // 4) % 4, k % 4
        here = (tz == z) & (tx == x) & (ty == y)

        @pl.when(here)
        def _():
            g_in[home_chip] = g_sum[k]

        @pl.when(jnp.logical_not(here))
        def _():
            pltpu.make_async_remote_copy(
                g_sum.at[k], g_in.at[home_chip], g_send, g_recv,
                device_id=device(tx, ty, tz, core), device_id_type=MESH,
            ).start()

        return carry

    lax.fori_loop(0, blocks, g_push, 0)

    def dispatched(chunk):
        first = 1 if chunk == 0 else 0
        many(size_in.at[pl.ds(first, PER - first)], disp_send.at[chunk]).wait()

    def go_home(chunk):
        def home(p, carry):
            for o in ORDER[chunk]:
                q = slot_of(*o)[1]
                pltpu.make_async_remote_copy(
                    two(rows, chunk, q, p), two(back, chunk, q, p),
                    back_send.at[chunk, q // 16], back_recv.at[chunk, q // 16],
                    device_id=peer(o, -1),
                    device_id_type=MESH,
                ).start()
            return carry

        lax.fori_loop(0, PAIRS, home, 0)

    forwards, swaps = [], []

    def pass_on(chunk):
        first = 1 if chunk == 0 else 0
        many(size_in.at[pl.ds(first, PER - first)], disp_recv.at[chunk]).wait()
        forward = pltpu.make_async_remote_copy(
            xs.at[chunk, pl.ds(0, HALF)], xs.at[chunk, pl.ds(HALF, HALF)],
            fwd_send.at[chunk], fwd_recv.at[chunk], device_id=partner, device_id_type=MESH,
        )
        forward.start()
        forwards.append(forward)

    for chunk in range(CHUNKS):
        if chunk == 0:
            pass_on(0)
        forward = forwards[chunk]
        if chunk == 0:
            loads[0].wait()
            loads[1].wait()
        forward.wait_recv()

        for n in range(gate_v.shape[1] // WIDE):
            cols = slice(n * WIDE, (n + 1) * WIDE)
            block = xs[chunk]
            gate = jnp.dot(block, gate_v[:, cols], preferred_element_type=F32)
            up = jnp.dot(block, up_v[:, cols], preferred_element_type=F32)
            hidden[:, cols] = (gate / (1.0 + jnp.exp(-gate)) * up).astype(BF16)
        if chunk == 0:
            loads[2].wait()

        for n, (start, size) in enumerate(PARTS):
            cols = slice(start, start + size)
            both = jnp.dot(hidden[...], down_v[:, cols], preferred_element_type=F32).astype(BF16)
            theirs[chunk, :, cols] = both[HALF:]
            mine[:, cols] = both[:HALF]
            swap = pltpu.make_async_remote_copy(
                theirs.at[chunk, :, pl.ds(start, size)], other.at[chunk, :, pl.ds(start, size)],
                out_send.at[chunk, n], out_recv.at[chunk, n],
                device_id=partner, device_id_type=MESH,
            )
            swap.start()
            swaps.append(swap)
        if chunk == 0:
            many(w_in.at[pl.ds(0, CHIPS - 1)], wt_recv).wait()
        spread = w_in[chunk * PER : (chunk + 1) * PER].reshape(PER, count)
        at = lax.broadcasted_iota(I32, (HALF, PER), 0)
        source = (((at * 205) >> 11) == lax.broadcasted_iota(I32, (HALF, PER), 1)).astype(F32)
        table = jnp.zeros((HALF, count), F32)
        for _ in range(3):
            piece = spread.astype(BF16)
            spread = spread - piece.astype(F32)
            table = table + jnp.dot(source.astype(BF16), piece, preferred_element_type=F32)
        at = lax.broadcasted_iota(I32, (HALF, count), 0)
        lane = lax.broadcasted_iota(I32, (HALF, count), 1)
        inside = at - ((at * 205) >> 11) * CAP
        even = jnp.sum(jnp.where(lane == inside, table, 0.0), axis=1, keepdims=True)
        odd = jnp.sum(jnp.where(lane == inside + 16, table, 0.0), axis=1, keepdims=True)
        is_even = (lax.broadcasted_iota(I32, even.shape, 0) * 0 + core) == 0
        w_mine = jnp.where(is_even, even, odd)
        w_other = jnp.where(is_even, odd, even)
        if chunk <= HOLD:
            dispatched(chunk)

        def sum_step(n, carry):
            cols = tile_at(n)
            rows[chunk, :, cols] = (
                w_mine * mine[:, cols].astype(F32) + w_other * other[chunk, :, cols].astype(F32)
            ).astype(BF16)
            return carry

        for n, (start, size) in enumerate(PARTS):
            swaps[chunk * len(PARTS) + n].wait_recv()
            lax.fori_loop(start // TILE, (start + size) // TILE, sum_step, 0)
        if chunk == 0:
            back[0, :CAP] = rows[0, :CAP]
        if chunk == HOLD:
            for later in range(chunk + 1, CHUNKS):
                dispatched(later)
        if chunk + 1 < CHUNKS:
            pass_on(chunk + 1)
        for ready in range(CHUNKS):
            if ready == chunk > HOLD or ready <= chunk == HOLD:
                go_home(ready)

    @pl.when(holder)
    def _():
        many(g_in.at[pl.ds(0, CHIPS - 1)], g_recv).wait()

        def g_fold(s, total):
            return total + g_in[s].astype(F32)

        g_tot[...] = lax.fori_loop(0, CHIPS, g_fold, jnp.zeros(g_tot.shape, F32))

        def g_give(k, carry):
            at = pl.multiple_of(k * 4, 4)
            pltpu.make_async_copy(
                g_tot.at[pl.ds(pl.multiple_of(core * 28 + k * 4, 4), 4)], router.at[pl.ds(at, 4)],
                g_out,
            ).start()
            pltpu.make_async_remote_copy(
                g_tot.at[pl.ds(pl.multiple_of((1 - core) * 28 + k * 4, 4), 4)],
                router.at[pl.ds(at, 4)], g_out_send, g_out_recv,
                device_id=partner, device_id_type=MESH,
            ).start()
            return carry

        lax.fori_loop(0, 7, g_give, 0)

    for step in range(CHUNKS * PARTIES):
        chunk, party = step // PARTIES, step % PARTIES
        first = 1 if step == 0 else 0
        many(size_in.at[pl.ds(first, 16 - first)], back_recv.at[chunk, party]).wait()
        lot = slice(party * 16 * CAP, (party + 1) * 16 * CAP)
        part = width // 4
        for k in range(4):
            cols = slice(k * part, (k + 1) * part)
            value = lax.dot_general(
                hot[chunk, lot], back[chunk, lot, cols], TURN, preferred_element_type=F32
            )
            if step:
                value = acc[:, cols] + value
            if step == CHUNKS * PARTIES - 1:
                mixed[:, cols] = value.astype(BF16)
            else:
                acc[:, cols] = value

    g_swap.wait_send()
    many(g_sum.at[pl.ds(0, blocks - 1)], g_send).wait()

    @pl.when(holder)
    def _():
        many(g_sum.at[0], g_out).wait()
        many(g_sum.at[0], g_out_send).wait()

    @pl.when(jnp.logical_not(holder))
    def _():
        many(g_sum.at[0], g_send).wait()
        many(g_sum.at[0], g_out_recv).wait()

    many(w_out.at[pl.ds(0, CHIPS - 1)], wt_send).wait()
    for chunk in range(CHUNKS):
        first = 1 if chunk == 0 else 0
        forwards[chunk].wait_send()
        for n in range(len(PARTS)):
            swaps[chunk * len(PARTS) + n].wait_send()
        for party in range(PARTIES):
            skip = first if party == 0 else 0
            many(size_in.at[pl.ds(skip, 16 - skip)], back_send.at[chunk, party]).wait()


def body(tokens, node_ids, local_ids, affinity, w_gate, w_up, w_down, grad_parts):
    count, width = tokens.shape
    inner = w_gate.shape[2]
    vmem = pl.BlockSpec(memory_space=pltpu.VMEM)
    hbm = pl.BlockSpec(memory_space=pltpu.HBM)
    dma = pltpu.SemaphoreType.DMA
    per_chunk = dma((CHUNKS,))
    blocks = CHIPS // 2
    deep = grad_parts.shape[1] // CHIPS
    lanes = grad_parts.shape[2]
    plain = jax.ShapeDtypeStruct((PER, PAIRS, 2, width), BF16)
    outs = pl.pallas_call(
        moe_body,
        name="moe",
        out_shape=(
            pltpu.VMEM((count, width), BF16),
            pltpu.VMEM((deep // 2, lanes), F32),
            plain,
        ),
        in_specs=[hbm] * 8,
        out_specs=(vmem, vmem, hbm),
        scratch_shapes=[
            pltpu.VMEM((4, count), I32),
            pltpu.VMEM((8, count), I32),
            pltpu.VMEM((8, count), F32),
            pltpu.VMEM((count, width), BF16),
            pltpu.VMEM((width, inner), BF16),
            pltpu.VMEM((width, inner), BF16),
            pltpu.VMEM((inner, width), BF16),
            pltpu.VMEM((CHUNKS, HALF, count), BF16),
            pltpu.VMEM((CHUNKS, HALF, width), BF16),
            pltpu.VMEM((CHUNKS, 2 * HALF, width), BF16),
            pltpu.VMEM((2 * HALF, inner), BF16),
            pltpu.VMEM((CHUNKS, HALF, width), BF16),
            pltpu.VMEM((HALF, width), BF16),
            pltpu.VMEM((CHUNKS, HALF, width), BF16),
            pltpu.VMEM((CHUNKS, HALF, width), BF16),
            pltpu.VMEM((count, width), F32),
            pltpu.VMEM((CHIPS, 1, count), F32),
            pltpu.VMEM((CHIPS, 1, count), F32),
            pltpu.VMEM((blocks, deep, lanes), F32),
            pltpu.VMEM((blocks, deep, lanes), F32),
            pltpu.VMEM((blocks, deep, lanes), BF16),
            pltpu.VMEM((CHIPS, deep, lanes), BF16),
            pltpu.VMEM((deep, lanes), F32),
            dma((4,)), dma((3,)),
            per_chunk, per_chunk, per_chunk, per_chunk,
            dma((CHUNKS, len(PARTS))), dma((CHUNKS, len(PARTS))),
            dma((CHUNKS, PARTIES)), dma((CHUNKS, PARTIES)), dma, dma,
            dma, dma, dma, dma, dma, dma, dma, dma,
        ],
        compiler_params=pltpu.CompilerParams(
            collective_id=0, has_side_effects=True, vmem_limit_bytes=64000000
        ),
        cost_estimate=pl.CostEstimate(
            flops=12 * CHIPS * CAP * width * inner, bytes_accessed=50 << 20, transcendentals=0
        ),
    )(
        node_ids.T, local_ids.T, affinity.T, tokens, w_gate, w_up, w_down,
        grad_parts.reshape(2, blocks, deep, lanes),
    )
    return outs[0], outs[1]


def solution(mesh):
    spec2 = P(("edp", "ep"), None)
    spec3 = P(("edp", "ep"), None, None)
    return jax.shard_map(
        body,
        mesh=mesh,
        in_specs=(spec2,) * 4 + (spec3,) * 4,
        out_specs=(spec2, spec2),
        check_vma=False,
    )
```
